256 devices in a mesh: dp: 16 (over z, x_hi), tensor: 16 (over y, x_lo, core).
Axes of the slice: x: 4 (x_hi: 2, x_lo: 2; x = x_hi * 2 + x_lo), y: 4, z: 8, core: 2. Of those that a mesh axis runs over, the one named last changes fastest.
Arguments:
- tokens: bfloat16 [16, 1024, 4096], P('dp', 'tensor'), may hold values from -6 to 6
- gain: bfloat16 [4096], replicated, may hold values from 0.5 to 1.5
- wq: bfloat16 [4096, 4096], P(None, 'tensor'), may hold values from -0.09375 to 0.09375
- bq: bfloat16 [4096], P('tensor'), may hold values from -5 to 5
- wkv: bfloat16 [4096, 1024], P(None, 'tensor'), may hold values from -0.09375 to 0.09375
- bkv: bfloat16 [1024], P('tensor'), may hold values from -5 to 5
- wo: bfloat16 [4096, 4096], P('tensor'), may hold values from -0.375 to 0.375
- check_weights: float32 [16, 1024], P('dp'), may hold values from -12 to 12
Outputs:
- attended: bfloat16 [16, 1024, 4096], P('dp', 'tensor')
- checksum: float32 [4096], replicated
The draws below stay inside these ranges and needn't reach their ends.
All inputs are finite; a program needn't handle non-finite values.
Results may differ from the reference program's by a relative error of at most 0.018.
Values may be sent and summed in bfloat16 or wider, within the bound.
A program may use at most 64 MiB of HBM per device.

```python
import jax
import jax.numpy as jnp
from jax import lax

D = 4096
HEADS = 32
KV = 4
HD = 128
SEQ = 1024
GROUPS = 16
N_TENSOR = 16


def draw_check_weights(key, part):
    rising = jnp.exp(jnp.log(3.0) * jnp.arange(GROUPS, dtype=jnp.float32) / max(GROUPS - 1, 1))
    base = jax.random.truncated_normal(key, -4.0, 4.0, (GROUPS, SEQ), jnp.float32)
    return (base * rising[:, None]).astype(jnp.float32)


def draw_bq(key, part):
    return (0.5 * jax.random.truncated_normal(jax.random.fold_in(key, 12), -6.0, 6.0, (HEADS * HD,), jnp.float32)).astype(jnp.bfloat16)


def draw_bkv(key, part):
    value_part = 0.5 * jax.random.truncated_normal(jax.random.fold_in(key, 13), -6.0, 6.0, (KV * HD,), jnp.float32)
    key_part = 0.5 * jax.random.truncated_normal(jax.random.fold_in(key, 15), -6.0, 6.0, (KV * HD,), jnp.float32)
    return jnp.concatenate([key_part, value_part], axis=0).astype(jnp.bfloat16)


def steps_of(own_key, dims, cuts, low, largest):
    loudness, own = 1.0, jax.random.fold_in(own_key, 6)
    for dim, parts in cuts:
        steps = jnp.exp(jax.random.uniform(jax.random.fold_in(own, dim), (parts,), jnp.float32, low / len(cuts), largest / len(cuts)))
        loudness = loudness * jnp.repeat(steps, dims[dim] // parts).reshape([-1 if axis == dim else 1 for axis in range(len(dims))])
    return loudness


def noise(stream_key, dims, width, bound, cuts=(), kind=jnp.bfloat16):
    level = steps_of(stream_key, dims, cuts, -0.22, 0.18) if cuts else 1.0
    entries = jax.random.normal(stream_key, dims, jnp.float32) * width * level
    return jnp.minimum(jnp.maximum(entries, -bound), bound).astype(kind)


def setup_inputs(seed: int = 0) -> dict:
    arg_keys = jax.random.split(jax.random.key(seed), 9)
    tokens = noise(arg_keys[0], (GROUPS, SEQ, D), 1.0, 6.0, ((0, 16), (1, 16)))
    gain = jnp.clip(1.0 + 0.1 * jax.random.normal(arg_keys[1], (D,), jnp.float32), 0.5, 1.5).astype(jnp.bfloat16)
    wq = noise(arg_keys[2], (D, HEADS * HD), D ** -0.5, 0.09375, ((1, 16),))
    bq = draw_bq(jax.random.fold_in(arg_keys[8], 71), 0)
    wkv = noise(arg_keys[4], (D, 2 * KV * HD), D ** -0.5, 0.09375, ((1, 16),))
    bkv = draw_bkv(jax.random.fold_in(arg_keys[8], 71), 0)
    wo = noise(arg_keys[6], (HEADS * HD, D), (HEADS * HD // 16) ** -0.5, 0.375, ((0, 16),))
    check_weights = draw_check_weights(jax.random.fold_in(arg_keys[8], 71), 0)
    return {"tokens": tokens, "gain": gain, "wq": wq, "bq": bq, "wkv": wkv, "bkv": bkv, "wo": wo, "check_weights": check_weights}


EPS = 1e-06
THETA = 1000000.0

def rope(values, head_size):
    rows = values.shape[0]
    half = head_size // 2
    inverse = THETA ** (-(jnp.arange(half, dtype=jnp.float32) * 2.0 / head_size))
    angles = jnp.arange(rows, dtype=jnp.float32)[:, None] * inverse[None, :]
    cosine = jnp.cos(angles)[:, None, :]
    sine = jnp.sin(angles)[:, None, :]
    shaped = values.reshape(rows, -1, head_size)
    first = shaped[..., :half]
    second = shaped[..., half:]
    turned = jnp.concatenate([first * cosine - second * sine, second * cosine + first * sine], axis=-1)
    return turned.reshape(rows, -1)

def reference(tokens, gain, wq, bq, wkv, bkv, wo, check_weights):
    per_dev = HEADS // N_TENSOR * HD
    ratio = HEADS // KV
    scale = HD ** (-0.5)
    causal = jnp.arange(SEQ)[:, None] >= jnp.arange(SEQ)[None, :]

    def one_group(inputs):
        tokens_g, weights_g = inputs
        states = tokens_g.astype(jnp.float32)
        normed = (states * lax.rsqrt(lax.optimization_barrier(jnp.mean(states * states, axis=-1, keepdims=True)) + EPS) * gain.astype(jnp.float32)).astype(jnp.bfloat16)
        query = rope(jnp.dot(normed, wq, preferred_element_type=jnp.float32) + bq.astype(jnp.float32), HD).astype(jnp.bfloat16)
        pairs = (jnp.dot(normed, wkv, preferred_element_type=jnp.float32) + bkv.astype(jnp.float32)).astype(jnp.bfloat16)
        keys = rope(pairs[:, :KV * HD].astype(jnp.float32), HD).astype(jnp.bfloat16)
        values = pairs[:, KV * HD:]

        def one_head(index):
            index = index.astype(jnp.int32)
            shared = (index // ratio).astype(jnp.int32)
            q_head = lax.dynamic_slice_in_dim(query, index * HD, HD, 1).astype(jnp.float32)
            k_head = lax.dynamic_slice_in_dim(keys, shared * HD, HD, 1).astype(jnp.float32)
            v_head = lax.dynamic_slice_in_dim(values, shared * HD, HD, 1).astype(jnp.float32)
            scores = jnp.dot(q_head, k_head.T, precision=lax.Precision.HIGHEST) * scale
            scores = jnp.where(causal, scores, -1e+30)
            probs = jax.nn.softmax(scores, axis=-1).astype(jnp.bfloat16)
            return jnp.dot(probs.astype(jnp.float32), v_head, precision=lax.Precision.HIGHEST).astype(jnp.bfloat16)
        heads_out = lax.map(one_head, jnp.arange(HEADS, dtype=jnp.int32))
        context = jnp.transpose(heads_out, (1, 0, 2)).reshape(SEQ, HEADS * HD)

        def add_part(total, index):
            index = index.astype(jnp.int32)
            piece = lax.dynamic_slice_in_dim(context, index * per_dev, per_dev, 1)
            rows = lax.dynamic_slice_in_dim(wo, index * per_dev, per_dev, 0)
            rounded = jnp.dot(piece, rows, preferred_element_type=jnp.float32).astype(jnp.bfloat16)
            rounded = lax.optimization_barrier(rounded)
            return (total + rounded.astype(jnp.float32), None)
        total, _ = lax.scan(add_part, jnp.zeros((SEQ, D), jnp.float32), jnp.arange(N_TENSOR, dtype=jnp.int32))
        summary = jnp.dot(weights_g, context.astype(jnp.float32), precision=lax.Precision.HIGHEST)
        term = jnp.dot(summary, wo.astype(jnp.float32), precision=lax.Precision.HIGHEST)
        return (total.astype(jnp.bfloat16), term)
    attended, terms = lax.map(one_group, (tokens, check_weights))
    checksum = lax.optimization_barrier(jnp.sum(terms, axis=0)) / jnp.sqrt(jnp.float32(SEQ * GROUPS))
    return (attended, checksum)
```

```python
import jax
import jax.numpy as jnp
import numpy as np
from jax import lax
from jax.experimental import pallas as pl
from jax.experimental.pallas import tpu as pltpu
from jax.sharding import Mesh
from jax.sharding import PartitionSpec as P

HD = 128
EPS = 1e-06
THETA = 1000000.0
TENSOR = ("tensor_0", "tensor_1", "tensor_2")
DP = ("dp_0", "dp_1")
MESH = pl.DeviceIdType.MESH
F32 = jnp.float32
BF16 = jnp.bfloat16

NY = 4
D = 4096
ROWS = 64
QUARTER = 16
QCOLS = 256
SEQ = 1024
CHUNKS = 8
CW = D // CHUNKS


def mult(value, by):
    return pl.multiple_of(value, by)


def split3(value):
    hi = value.astype(BF16).astype(F32)
    rest = value - hi
    mid = rest.astype(BF16).astype(F32)
    low = (rest - mid).astype(BF16).astype(F32)
    row = lax.broadcasted_iota(jnp.int32, (16, value.shape[1]), 0)
    rows = jnp.where(row == 0, hi, jnp.where(row == 1, mid, jnp.where(row == 2, low, 0.0)))
    return rows.astype(BF16)


def kernel(
    tokens, params, wq, wkv, wo, weights, cos, sin,
    out, check,
    tok, xg, wqv, wkown, wkpair, wkfull, bpair, cosv, sinv, qb, kvs, kv, ctx, ctx4, wo4,
    pbuf, ra, rfb, rfa, outv, cz, chh, cxl, cc, cy,
    ld, wl, agr, agd, ags, agds, wkr, wks, wor, wos, wod, wods,
    kvr, kvd, kvss, kvds, cxr, cxs, rar, ras, rbr, rbs, rtr, rts, ost,
    czr, czs, cdr, cds,
):
    z = lax.axis_index("dp_0")
    xh = lax.axis_index("dp_1")
    y = lax.axis_index("tensor_0")
    x = lax.axis_index("tensor_1")
    c = lax.axis_index("tensor_2")
    slot = x * 2 + c
    other_x = (x + 1) % 2
    other_c = (c + 1) % 2

    def at(dy=0, dx=0, dc=0):
        return {"tensor_0": (y + dy) % NY, "tensor_1": (x + dx) % 2, "tensor_2": (c + dc) % 2}

    def unit(dy, dx):
        return ((y + dy) % NY) * 2 + (x + dx) % 2

    up, down, pair, sibling = at(dy=1), at(dy=3), at(dx=1), at(dc=1)
    far = {"dp_1": (xh + 1) % 2, "tensor_1": other_x}

    barrier = pltpu.get_barrier_semaphore()
    peers = [at(dy=dy, dx=dx) for dy in range(4) for dx in range(2) if dy or dx]
    peers += [sibling, at(dx=1, dc=1), far, {"dp_1": (xh + 1) % 2}]
    peers += [{"dp_0": (z + d) % 8} for d in range(1, 8)]
    for peer in peers:
        pl.semaphore_signal(barrier, inc=1, device_id=peer, device_id_type=MESH)

    loads = {}

    def load(name, src, dst, sem):
        loads[name] = pltpu.make_async_copy(src, dst, sem)
        loads[name].start()

    load("tok", tokens, tok, ld.at[0])
    load("wk", wkv, wkown, ld.at[1])
    load("wq", wq, wqv, ld.at[2])
    load("cos", cos, cosv, ld.at[3])
    load("sin", sin, sinv, ld.at[4])
    my_wo = pl.ds(mult(slot * QCOLS, QCOLS), QCOLS)
    for j in range(CHUNKS):
        load(("wo", j), wo.at[:, pl.ds(j * CW, CW)], wo4.at[j, my_wo, :], wl.at[j])

    pending = []

    def send(src, dst, ssem, rsem, device):
        copy = pltpu.make_async_remote_copy(
            src_ref=src, dst_ref=dst, send_sem=ssem, recv_sem=rsem,
            device_id=device, device_id_type=MESH,
        )
        copy.start()
        pending.append(copy)

    def arrived(dst, ssem, rsem, device):
        pltpu.make_async_remote_copy(
            src_ref=dst, dst_ref=dst, send_sem=ssem, recv_sem=rsem,
            device_id=device, device_id_type=MESH,
        ).wait_recv()

    gain = params[0:1, 0:D]
    base = (y * 4 + slot) * ROWS
    loads["tok"].wait()
    for q in range(4):
        part = tok[q * QUARTER:(q + 1) * QUARTER, :].astype(F32)
        mean = jnp.mean(part * part, axis=-1, keepdims=True)
        xg[pl.ds(mult(base + q * QUARTER, QUARTER), QUARTER), :] = (
            part * lax.rsqrt(mean + EPS) * gain
        ).astype(BF16)

    pl.semaphore_wait(barrier, len(peers))

    def piece(u, q):
        return xg.at[pl.ds(mult(u * 128 + c * ROWS + q * QUARTER, QUARTER), QUARTER), :]

    def sibling_piece(u, q):
        return xg.at[pl.ds(mult(u * 128 + other_c * ROWS + q * QUARTER, QUARTER), QUARTER), :]

    counts = {"ags": 0, "agds": 0}

    def relay(u, q, device):
        k = counts["ags"]
        counts["ags"] += 1
        send(piece(u, q), piece(u, q), ags.at[k], agr.at[u * 4 + q], device)

    def relay_sibling(u, q):
        k = counts["agds"]
        counts["agds"] += 1
        send(piece(u, q), piece(u, q), agds.at[k], agd.at[u * 4 + q], sibling)

    def wait_piece(u, q):
        arrived(piece(u, q), ags.at[0], agr.at[u * 4 + q], sibling)

    def wait_sibling(u):
        for q in range(4):
            arrived(sibling_piece(u, q), agds.at[0], agd.at[u * 4 + q], sibling)

    own = unit(0, 0)
    for s in range(4):
        relay(own, s, up)
        relay(own, (s + 2) % 4, down)
        relay(own, s, pair)
    for q in range(4):
        relay_sibling(own, q)

    loads["wk"].wait()
    send(wkown, wkpair, wks.at[0], wkr.at[0], sibling)
    send(params.at[:, pl.ds(D + QCOLS, 128)], bpair, wks.at[1], wkr.at[1], sibling)

    def wo_piece(j, owner):
        return wo4.at[j, pl.ds(mult(owner * QCOLS, QCOLS), QCOLS), :]

    for j in range(CHUNKS):
        loads[("wo", j)].wait()
        send(wo_piece(j, slot), wo_piece(j, slot), wos.at[j], wor.at[j], far)
        send(wo_piece(j, slot), wo_piece(j, slot), wods.at[j], wod.at[j], sibling)

    far_slot = other_x * 2 + c
    sibling_slot = x * 2 + other_c
    far_sibling_slot = other_x * 2 + other_c

    def forward_wo(j):
        arrived(wo_piece(j, far_slot), wos.at[j], wor.at[j], far)
        send(wo_piece(j, far_slot), wo_piece(j, far_slot), wods.at[8 + j], wod.at[8 + j], sibling)

    arrived(wkpair, wks.at[0], wkr.at[0], sibling)
    arrived(bpair, wks.at[1], wkr.at[1], sibling)
    first = c == 0

    def join(i, carry):
        rows = pl.ds(mult(i * 512, 512), 512)
        mine, theirs = wkown[rows, :], wkpair[rows, :]
        left = jnp.where(first, mine, theirs)
        right = jnp.where(first, theirs, mine)
        wkfull[rows, :] = jnp.concatenate([left, right], axis=1)
        return carry

    lax.fori_loop(0, D // 512, join, 0)
    lane = lax.broadcasted_iota(jnp.int32, (1, 128), 1)
    bias_mine = params[0:1, D + QCOLS:D + QCOLS + 128]
    bias_theirs = bpair[0:1, :]
    low_half = lane < 64
    kv_bias = jnp.where(
        first,
        jnp.where(low_half, bias_mine, bias_theirs),
        jnp.where(low_half, bias_theirs, bias_mine),
    )
    q_bias = params[0:1, D:D + QCOLS]
    loads["wq"].wait()
    loads["cos"].wait()
    loads["sin"].wait()

    chip = y * 2 + x
    is_value = y // 2
    turned = (1 - is_value).astype(F32)
    straight = is_value.astype(F32)
    group = chip % NY
    local_user = group == y
    local_sends = []

    def rope(value, cosine, sine):
        return value * cosine + pltpu.roll(value, 64, 1) * sine

    def project(step, u):
        rows_kv = pl.ds(mult(u * 128 + c * ROWS, ROWS), ROWS)
        pairs = jnp.dot(xg[rows_kv, :], wkfull[...], preferred_element_type=F32) + kv_bias
        pairs = pairs.astype(BF16).astype(F32)
        cosine = cosv[rows_kv, :] * turned + straight
        sine = sinv[rows_kv, :] * turned
        result = rope(pairs, cosine, sine).astype(BF16)
        kvs[step] = result
        target = kv.at[is_value, rows_kv, :]
        sem = kvr.at[is_value * 8 + u]
        same = pltpu.make_async_remote_copy(
            src_ref=kvs.at[step], dst_ref=target, send_sem=kvss.at[step], recv_sem=sem,
            device_id={"tensor_0": group}, device_id_type=MESH,
        )

        @pl.when(local_user)
        def _():
            kv[is_value, rows_kv, :] = result

        @pl.when(jnp.logical_not(local_user))
        def _():
            same.start()

        local_sends.append(same)
        send(kvs.at[step], target, kvss.at[8 + step], sem, {"tensor_0": group, "tensor_1": other_x})

        rows = pl.ds(mult(u * 128, 128), 128)
        query = jnp.dot(xg[rows, :], wqv[...], preferred_element_type=F32) + q_bias
        for h in range(2):
            cols = slice(h * HD, (h + 1) * HD)
            qb[rows, cols] = rope(query[:, cols], cosv[rows, :], sinv[rows, :]).astype(BF16)

    below, above, beside, across = unit(3, 0), unit(1, 0), unit(0, 1), unit(2, 0)
    x_across, x_below, x_above = unit(2, 1), unit(3, 1), unit(1, 1)

    wait_sibling(own)
    project(0, own)
    for s in range(4):
        wait_piece(below, s)
        if s < 2:
            relay(below, s, up)
        r = (s + 2) % 4
        wait_piece(above, r)
        if s < 2:
            relay(above, r, down)
        wait_piece(beside, s)
        relay(beside, s, up)
        relay(beside, s, down)
        relay_sibling(below, s)
        relay_sibling(above, r)
        relay_sibling(beside, s)
    wait_sibling(below)
    project(1, below)
    for q in (0, 2):
        wait_piece(across, q)
        relay(across, q, pair)
        relay_sibling(across, q)
    forward_wo(0)
    wait_sibling(above)
    project(2, above)
    for u in (x_below, x_above):
        wait_piece(u, 0)
        relay_sibling(u, 0)
    forward_wo(1)
    wait_sibling(beside)
    project(3, beside)
    for q in (1, 3):
        wait_piece(across, q)
        relay(across, q, pair)
        relay_sibling(across, q)
    for q in (0, 2):
        wait_piece(x_across, q)
        relay_sibling(x_across, q)
    for u in (x_below, x_above):
        wait_piece(u, 1)
        relay_sibling(u, 1)
    wait_sibling(across)
    project(4, across)
    forward_wo(2)
    for u in (x_below, x_above):
        wait_piece(u, 2)
        relay_sibling(u, 2)
    for q in (1, 3):
        wait_piece(x_across, q)
        relay_sibling(x_across, q)
    wait_sibling(x_across)
    project(5, x_across)
    for u in (x_below, x_above):
        wait_piece(u, 3)
        relay_sibling(u, 3)
    forward_wo(3)
    wait_sibling(x_below)
    project(6, x_below)
    wait_sibling(x_above)
    project(7, x_above)

    made_here = [
        jnp.logical_and(y == 0, x == 0),
        jnp.logical_and(y == 3, x == 1),
    ]
    for u in range(8):
        for kind in range(2):
            rows_kv = pl.ds(mult(u * 128 + c * ROWS, ROWS), ROWS)
            part = kv.at[kind, rows_kv, :]

            @pl.when(jnp.logical_not(made_here[kind]))
            def _():
                arrived(part, kvss.at[0], kvr.at[kind * 8 + u], sibling)

            send(part, part, kvds.at[kind * 8 + u], kvd.at[kind * 8 + u], sibling)
    for u in range(8):
        for kind in range(2):
            rows_kv = pl.ds(mult(u * 128 + other_c * ROWS, ROWS), ROWS)
            arrived(kv.at[kind, rows_kv, :], kvds.at[0], kvd.at[kind * 8 + u], sibling)

    forward_wo(4)

    scale = HD ** (-0.5)
    my_cols = pl.ds(mult(slot * QCOLS, QCOLS), QCOLS)
    contract_last = (((1,), (1,)), ((), ()))
    for b in reversed(range(4)):
        block = slice(b * 256, (b + 1) * 256)
        row = lax.broadcasted_iota(jnp.int32, (256, 256), 0)
        col = lax.broadcasted_iota(jnp.int32, (256, 256), 1)
        for h in range(2):
            cols = slice(h * HD, (h + 1) * HD)
            query = qb[block, cols]
            diagonal = lax.dot_general(query, kv[0, block, :], contract_last, preferred_element_type=F32)
            diagonal = jnp.where(row >= col, diagonal, -1e30)
            top = jnp.max(diagonal, axis=-1, keepdims=True)
            if b:
                earlier = lax.dot_general(
                    query, kv[0, 0:b * 256, :], contract_last, preferred_element_type=F32
                )
                top = jnp.maximum(top, jnp.max(earlier, axis=-1, keepdims=True))
            weight = jnp.exp((diagonal - top) * scale)
            total = jnp.sum(weight, axis=-1, keepdims=True)
            mixed = jnp.dot(weight.astype(BF16), kv[1, block, :], preferred_element_type=F32)
            if b:
                weight = jnp.exp((earlier - top) * scale)
                total += jnp.sum(weight, axis=-1, keepdims=True)
                mixed += jnp.dot(weight.astype(BF16), kv[1, 0:b * 256, :], preferred_element_type=F32)
            ctx[block, cols] = (mixed / total).astype(BF16)
        target = pl.ds(b * ROWS, ROWS)
        ctx4[target, my_cols] = ctx[pl.ds(mult(b * 256 + slot * ROWS, ROWS), ROWS), :]
        for k, (dx, dc) in enumerate(((1, 0), (1, 1), (0, 1))):
            theirs = ((x + dx) % 2) * 2 + (c + dc) % 2
            send(
                ctx.at[pl.ds(mult(b * 256 + theirs * ROWS, ROWS), ROWS), :],
                ctx4.at[target, my_cols],
                cxs.at[k * 4 + b], cxr.at[k * 4 + b], at(dx=dx, dc=dc),
            )

    summary = jnp.dot(split3(weights[0:1, :]), ctx[...], preferred_element_type=F32)
    summary = jnp.sum(summary, axis=0, keepdims=True)
    ctx4[256:272, :] = jnp.zeros((16, SEQ), BF16)
    ctx4[256:272, my_cols] = split3(summary)

    forward_wo(5)
    for k, (dx, dc) in enumerate(((1, 0), (1, 1), (0, 1))):
        theirs = ((x + dx) % 2) * 2 + (c + dc) % 2
        cols = pl.ds(mult(theirs * QCOLS, QCOLS), QCOLS)
        for b in range(4):
            arrived(
                ctx4.at[b * ROWS:(b + 1) * ROWS, cols], cxs.at[0], cxr.at[k * 4 + b], at(dx=dx, dc=dc)
            )

    def target_rows(dy):
        return pl.ds(mult(((y + dy) % NY) * ROWS, ROWS), ROWS)

    for j in range(CHUNKS):
        if j + 2 < CHUNKS and j + 2 > 5:
            forward_wo(j + 2)
        arrived(wo_piece(j, sibling_slot), wods.at[0], wod.at[j], sibling)
        arrived(wo_piece(j, far_sibling_slot), wods.at[0], wod.at[8 + j], sibling)
        product = jnp.dot(ctx4[...], wo4[j], preferred_element_type=F32)
        pbuf[j] = product[0:256, :].astype(BF16)
        cz[z, j:j + 1, :] = jnp.sum(product[256:272, :], axis=0, keepdims=True)
        if j % 2 == 0:
            send(pbuf.at[j, target_rows(2), :], ra.at[j], ras.at[j], rar.at[j], up)
            send(pbuf.at[j, target_rows(3), :], rfa.at[j], rts.at[j], rtr.at[j], down)
        else:
            send(pbuf.at[j, target_rows(2), :], ra.at[j], ras.at[j], rar.at[j], down)
            send(pbuf.at[j, target_rows(1), :], rfb.at[j], rbs.at[j], rbr.at[j], up)

    stages = [
        ("dp_0", 8, z, cz, 0),
        ("dp_1", 2, xh, chh, 0),
        ("tensor_1", 2, x, cxl, 1),
        ("tensor_2", 2, c, cc, 2),
        ("tensor_0", 4, y, cy, 3),
    ]

    def stage_start(i):
        axis, size, index, buf, first_sem = stages[i]
        for d in range(1, size):
            ssem, rsem = (czs.at[d], czr.at[d]) if i == 0 else (cds.at[first_sem + d - 1], cdr.at[first_sem + d - 1])
            send(buf.at[index], buf.at[index], ssem, rsem, {axis: (index + d) % size})

    def stage_end(i):
        axis, size, index, buf, first_sem = stages[i]
        for d in range(1, size):
            ssem, rsem = (czs.at[d], czr.at[d]) if i == 0 else (cds.at[first_sem + d - 1], cdr.at[first_sem + d - 1])
            source = (index + size - d) % size
            arrived(buf.at[source], ssem, rsem, {axis: source})
        total = buf[0]
        for k in range(1, size):
            total = total + buf[k]
        if i + 1 < len(stages):
            stages[i + 1][3][stages[i + 1][2]] = total
        else:
            check[...] = total * (1.0 / 128.0)

    stage_start(0)
    for j in range(CHUNKS):
        rows = target_rows(1 if j % 2 == 0 else 3)
        arrived(ra.at[j], ras.at[j], rar.at[j], sibling)
        pbuf[j, rows, :] = (pbuf[j, rows, :].astype(F32) + ra[j].astype(F32)).astype(BF16)
        if j % 2 == 0:
            send(pbuf.at[j, rows, :], rfb.at[j], rbs.at[j], rbr.at[j], up)
        else:
            send(pbuf.at[j, rows, :], rfa.at[j], rts.at[j], rtr.at[j], down)
        if j % 2 == 1:
            stage_end(j // 2)
            stage_start(j // 2 + 1)

    mine = target_rows(0)
    stores = []
    for j in (1, 3, 5, 7, 0, 2, 4, 6):
        arrived(rfb.at[j], rbs.at[j], rbr.at[j], sibling)
        arrived(rfa.at[j], rts.at[j], rtr.at[j], sibling)
        total = pbuf[j, mine, :].astype(F32) + rfb[j].astype(F32) + rfa[j].astype(F32)
        cols = slice(j * CW, (j + 1) * CW)
        outv[:, cols] = total.astype(BF16)
        store = pltpu.make_async_copy(outv.at[:, cols], out.at[:, cols], ost.at[j])
        store.start()
        stores.append(store)
    stage_end(4)

    for store in stores:
        store.wait()
    for copy in pending:
        copy.wait_send()
    for copy in local_sends:
        @pl.when(jnp.logical_not(local_user))
        def _():
            copy.wait_send()


def tables():
    half = HD // 2
    inverse = THETA ** (-(np.arange(half, dtype=np.float64) * 2.0 / HD))
    angles = np.arange(SEQ, dtype=np.float64)[:, None] * inverse[None, :]
    cosine, sine = np.cos(angles), np.sin(angles)
    return (
        np.concatenate([cosine, cosine], axis=1).astype(np.float32),
        np.concatenate([-sine, sine], axis=1).astype(np.float32),
    )


def local(tokens, gain, wq, bq, wkv, bkv, wo, check_weights):
    params = jnp.concatenate([gain, bq, bkv, bkv]).astype(F32)
    params = jnp.broadcast_to(params[None, :], (8, params.shape[0]))
    cosine, sine = tables()
    dma = pltpu.SemaphoreType.DMA
    vmem = pltpu.VMEM
    anywhere = pl.BlockSpec(memory_space=pl.ANY)
    inside = pl.BlockSpec(memory_space=pltpu.VMEM)
    attended, total = pl.pallas_call(
        kernel,
        out_shape=(
            jax.ShapeDtypeStruct((ROWS, D), BF16),
            jax.ShapeDtypeStruct((CHUNKS, CW), F32),
        ),
        in_specs=[anywhere, inside, anywhere, anywhere, anywhere, inside, anywhere, anywhere],
        out_specs=(anywhere, inside),
        scratch_shapes=[
            vmem((ROWS, D), BF16),
            vmem((SEQ, D), BF16),
            vmem((D, QCOLS), BF16),
            vmem((D, 64), BF16),
            vmem((D, 64), BF16),
            vmem((D, 128), BF16),
            vmem((8, 128), F32),
            vmem((SEQ, HD), F32),
            vmem((SEQ, HD), F32),
            vmem((SEQ, QCOLS), BF16),
            vmem((8, ROWS, HD), BF16),
            vmem((2, SEQ, HD), BF16),
            vmem((SEQ, QCOLS), BF16),
            vmem((272, SEQ), BF16),
            vmem((CHUNKS, SEQ, CW), BF16),
            vmem((CHUNKS, 256, CW), BF16),
            vmem((CHUNKS, ROWS, CW), BF16),
            vmem((CHUNKS, ROWS, CW), BF16),
            vmem((CHUNKS, ROWS, CW), BF16),
            vmem((ROWS, D), BF16),
            vmem((8, CHUNKS, CW), F32),
            vmem((2, CHUNKS, CW), F32),
            vmem((2, CHUNKS, CW), F32),
            vmem((2, CHUNKS, CW), F32),
            vmem((4, CHUNKS, CW), F32),
            dma((5,)), dma((8,)), dma((32,)), dma((32,)), dma((28,)), dma((32,)),
            dma((2,)), dma((2,)), dma((8,)), dma((8,)), dma((16,)), dma((16,)),
            dma((16,)), dma((16,)), dma((16,)), dma((16,)), dma((12,)), dma((12,)),
            dma((8,)), dma((8,)), dma((8,)), dma((8,)), dma((8,)), dma((8,)), dma((8,)),
            dma((8,)), dma((8,)), dma((6,)), dma((6,)),
        ],
        compiler_params=pltpu.CompilerParams(
            collective_id=0, has_side_effects=True, vmem_limit_bytes=56 * 1024 * 1024
        ),
        name="sublayer",
    )(tokens[0], params, wq, wkv, wo, check_weights, cosine, sine)
    return attended[None], total.reshape(D)


def solution(mesh):
    torus = Mesh(
        mesh.devices.reshape(8, 2, 4, 2, 2), ("dp_0", "dp_1", "tensor_0", "tensor_1", "tensor_2")
    )
    return jax.shard_map(
        local,
        mesh=torus,
        in_specs=(
            P(DP, TENSOR, None),
            P(),
            P(None, TENSOR),
            P(TENSOR),
            P(None, TENSOR),
            P(TENSOR),
            P(TENSOR, None),
            P(DP, None),
        ),
        out_specs=(P(DP, TENSOR, None), P()),
        check_vma=False,
    )
```

```python
import jax
import jax.numpy as jnp
import numpy as np
from jax import lax
from jax.experimental import pallas as pl
from jax.experimental.pallas import tpu as pltpu
from jax.sharding import Mesh
from jax.sharding import PartitionSpec as P

HD = 128
EPS = 1e-06
THETA = 1000000.0
TENSOR = ("tensor_0", "tensor_1", "tensor_2")
DP = ("dp_0", "dp_1")
MESH = pl.DeviceIdType.MESH
F32 = jnp.float32
BF16 = jnp.bfloat16

NY = 4
D = 4096
ROWS = 64
QUARTER = 16
QCOLS = 256
SEQ = 1024
CHUNKS = 8
CW = D // CHUNKS
NEAR_CHUNK = 7
LATE = 5


def mult(value, by):
    return pl.multiple_of(value, by)


def split3(value):
    hi = value.astype(BF16).astype(F32)
    rest = value - hi
    mid = rest.astype(BF16).astype(F32)
    low = (rest - mid).astype(BF16).astype(F32)
    row = lax.broadcasted_iota(jnp.int32, (16, value.shape[1]), 0)
    rows = jnp.where(row == 0, hi, jnp.where(row == 1, mid, jnp.where(row == 2, low, 0.0)))
    return rows.astype(BF16)


def kernel(
    tokens, gain_in, bq_in, bkv_in, wq, wkv, wo, weights, cos, sin,
    out, check,
    tok, xg, wqv, wkfull, bmine, bpair, cosv, sinv, qb, kvs, kv, ctx, ctx4, wo4,
    pbuf, ra, rfb, rfa, outv, cz, chh, cxl, cc, cy,
    ld, tl, wl, agr, agd, ags, agds, wkr, wks, wor, wos, wod, wods,
    kvr, kvd, kvss, kvds, cxr, cxs, rar, ras, rbr, rbs, rtr, rts, ost,
    cdr, cds,
):
    z = lax.axis_index("dp_0")
    xh = lax.axis_index("dp_1")
    y = lax.axis_index("tensor_0")
    x = lax.axis_index("tensor_1")
    c = lax.axis_index("tensor_2")
    slot = x * 2 + c
    other_x = (x + 1) % 2
    other_c = (c + 1) % 2

    def at(dy=0, dx=0, dc=0):
        return {"tensor_0": (y + dy) % NY, "tensor_1": (x + dx) % 2, "tensor_2": (c + dc) % 2}

    def unit(dy, dx):
        return ((y + dy) % NY) * 2 + (x + dx) % 2

    up, down, pair, sibling = at(dy=1), at(dy=3), at(dx=1), at(dc=1)
    far = {"dp_1": (xh + 1) % 2, "tensor_1": other_x}

    barrier = pltpu.get_barrier_semaphore()
    peers = [at(dy=dy, dx=dx) for dy in range(4) for dx in range(2) if dy or dx]
    peers += [sibling, at(dx=1, dc=1), far, {"dp_1": (xh + 1) % 2}]
    peers += [{"dp_0": (z + d) % 8} for d in range(1, 8)]
    for peer in peers:
        pl.semaphore_signal(barrier, inc=1, device_id=peer, device_id_type=MESH)

    contract_last = (((1,), (1,)), ((), ()))
    loads = {}

    def load(name, src, dst, sem):
        loads[name] = pltpu.make_async_copy(src, dst, sem)
        loads[name].start()

    for q in range(4):
        part = slice(q * QUARTER, (q + 1) * QUARTER)
        load(("tok", q), tokens.at[part, :], tok.at[part, :], tl.at[q])
    my_wk = wkfull.at[pl.ds(mult(c * 64, 64), 64), :]
    load("wk", wkv, my_wk, ld.at[1])
    load("wq", wq, wqv, ld.at[2])
    load("cos", cos, cosv, ld.at[3])
    load("sin", sin, sinv, ld.at[4])
    my_wo = pl.ds(mult(slot * QCOLS, QCOLS), QCOLS)
    for j in range(CHUNKS):
        load(("wo", j), wo.at[:, pl.ds(j * CW, CW)], wo4.at[j, my_wo, :], wl.at[j])

    pending = []

    def send(src, dst, ssem, rsem, device):
        copy = pltpu.make_async_remote_copy(
            src_ref=src, dst_ref=dst, send_sem=ssem, recv_sem=rsem,
            device_id=device, device_id_type=MESH,
        )
        copy.start()
        pending.append(copy)

    def arrived(dst, ssem, rsem, device):
        pltpu.make_async_remote_copy(
            src_ref=dst, dst_ref=dst, send_sem=ssem, recv_sem=rsem,
            device_id=device, device_id_type=MESH,
        ).wait_recv()

    gain = gain_in[...].astype(F32).reshape(1, D)
    q_bias = bq_in[...].astype(F32).reshape(1, QCOLS)
    bias_mine = bkv_in[...].astype(F32).reshape(1, 64)
    bias_mine = jnp.concatenate([bias_mine, bias_mine], axis=1)
    bmine[...] = jnp.broadcast_to(bias_mine, (8, 128))
    base = (y * 4 + slot) * ROWS
    for q in range(4):
        loads[("tok", q)].wait()
        part = tok[q * QUARTER:(q + 1) * QUARTER, :].astype(F32)
        mean = jnp.mean(part * part, axis=-1, keepdims=True)
        xg[pl.ds(mult(base + q * QUARTER, QUARTER), QUARTER), :] = (
            part * lax.rsqrt(mean + EPS) * gain
        ).astype(BF16)

    pl.semaphore_wait(barrier, len(peers))

    def piece(u, q):
        return xg.at[pl.ds(mult(u * 128 + c * ROWS + q * QUARTER, QUARTER), QUARTER), :]

    def sibling_piece(u, q):
        return xg.at[pl.ds(mult(u * 128 + other_c * ROWS + q * QUARTER, QUARTER), QUARTER), :]

    counts = {"ags": 0, "agds": 0}

    def relay(u, q, device):
        k = counts["ags"]
        counts["ags"] += 1
        send(piece(u, q), piece(u, q), ags.at[k], agr.at[u * 4 + q], device)

    def relay_sibling(u, q):
        k = counts["agds"]
        counts["agds"] += 1
        send(piece(u, q), piece(u, q), agds.at[k], agd.at[u * 4 + q], sibling)

    def wait_piece(u, q):
        arrived(piece(u, q), ags.at[0], agr.at[u * 4 + q], sibling)

    def wait_sibling(u):
        for q in range(4):
            arrived(sibling_piece(u, q), agds.at[0], agd.at[u * 4 + q], sibling)

    own = unit(0, 0)
    for s in range(4):
        relay(own, s, up)
        relay(own, (s + 2) % 4, down)
        relay(own, s, pair)
    for q in range(4):
        relay_sibling(own, q)

    loads["wk"].wait()
    send(my_wk, my_wk, wks.at[0], wkr.at[0], sibling)
    send(bmine, bpair, wks.at[1], wkr.at[1], sibling)

    def wo_piece(j, owner):
        return wo4.at[j, pl.ds(mult(owner * QCOLS, QCOLS), QCOLS), :]

    for j in range(CHUNKS):
        loads[("wo", j)].wait()
        route = pair if j == NEAR_CHUNK else far
        send(wo_piece(j, slot), wo_piece(j, slot), wos.at[j], wor.at[j], route)
        send(wo_piece(j, slot), wo_piece(j, slot), wods.at[j], wod.at[j], sibling)

    far_slot = other_x * 2 + c
    sibling_slot = x * 2 + other_c
    far_sibling_slot = other_x * 2 + other_c

    def forward_wo(j):
        arrived(wo_piece(j, far_slot), wos.at[j], wor.at[j], far)
        send(wo_piece(j, far_slot), wo_piece(j, far_slot), wods.at[8 + j], wod.at[8 + j], sibling)

    arrived(wkfull.at[pl.ds(mult(other_c * 64, 64), 64), :], wks.at[0], wkr.at[0], sibling)
    arrived(bpair, wks.at[1], wkr.at[1], sibling)
    first = c == 0
    lane = lax.broadcasted_iota(jnp.int32, (1, 128), 1)
    bias_theirs = bpair[0:1, :]
    low_half = lane < 64
    kv_bias = jnp.where(
        first,
        jnp.where(low_half, bias_mine, bias_theirs),
        jnp.where(low_half, bias_theirs, bias_mine),
    )
    loads["wq"].wait()
    loads["cos"].wait()
    loads["sin"].wait()

    chip = y * 2 + x
    is_value = y // 2
    turned = (1 - is_value).astype(F32)
    straight = is_value.astype(F32)
    group = chip % NY
    local_user = group == y
    local_sends = []

    def rope(value, cosine, sine):
        return value * cosine + pltpu.roll(value, 64, 1) * sine

    def plane_rows(u, plane):
        return pl.ds(mult(u * 128 + plane * ROWS, ROWS), ROWS)

    made = {"count": 0}

    def push(step, rows_kv, sem, device):
        k = made["count"]
        made["count"] += 1
        return pltpu.make_async_remote_copy(
            src_ref=kvs.at[step], dst_ref=kv.at[is_value, rows_kv, :],
            send_sem=kvss.at[k], recv_sem=sem, device_id=device, device_id_type=MESH,
        )

    def make_pairs(steps, units):
        lhs = [xg[plane_rows(u, c), :] for u in units]
        lhs = lhs[0] if len(lhs) == 1 else jnp.concatenate(lhs, axis=0)
        made_rows = lax.dot_general(
            lhs, wkfull[...], contract_last, preferred_element_type=F32
        ) + kv_bias
        made_rows = made_rows.astype(BF16).astype(F32)
        for i, (step, u) in enumerate(zip(steps, units)):
            rows_kv = plane_rows(u, c)
            cosine = cosv[rows_kv, :] * turned + straight
            sine = sinv[rows_kv, :] * turned
            result = rope(made_rows[i * ROWS:(i + 1) * ROWS, :], cosine, sine).astype(BF16)
            kvs[step] = result
            sem = kvr.at[is_value * 8 + u]
            same = push(step, rows_kv, sem, {"tensor_0": group})

            @pl.when(local_user)
            def _():
                kv[is_value, rows_kv, :] = result

            @pl.when(jnp.logical_not(local_user))
            def _():
                same.start()

            local_sends.append(same)
            others = [push(step, rows_kv, sem, {"tensor_0": group, "tensor_1": other_x})]
            if step >= LATE:
                sem = kvd.at[is_value * 8 + u]
                for px in (other_x, x):
                    others.append(
                        push(step, rows_kv, sem, {"tensor_0": group, "tensor_1": px, "tensor_2": other_c})
                    )
            for copy in others:
                copy.start()
                pending.append(copy)

    def make_query(units):
        lhs = [xg[pl.ds(mult(u * 128, 128), 128), :] for u in units]
        lhs = lhs[0] if len(lhs) == 1 else jnp.concatenate(lhs, axis=0)
        query = jnp.dot(lhs, wqv[...], preferred_element_type=F32) + q_bias
        for i, u in enumerate(units):
            rows = pl.ds(mult(u * 128, 128), 128)
            for h in range(2):
                cols = slice(h * HD, (h + 1) * HD)
                part = query[i * 128:(i + 1) * 128, cols]
                qb[rows, cols] = rope(part, cosv[rows, :], sinv[rows, :]).astype(BF16)

    def project(step, u):
        wait_sibling(u)
        make_pairs([step], [u])
        make_query([u])

    below, above, beside, across = unit(3, 0), unit(1, 0), unit(0, 1), unit(2, 0)
    x_across, x_below, x_above = unit(2, 1), unit(3, 1), unit(1, 1)

    project(0, own)
    for s in range(4):
        wait_piece(below, s)
        if s < 2:
            relay(below, s, up)
        r = (s + 2) % 4
        wait_piece(above, r)
        if s < 2:
            relay(above, r, down)
        wait_piece(beside, s)
        relay(beside, s, up)
        relay(beside, s, down)
        relay_sibling(below, s)
        relay_sibling(above, r)
        relay_sibling(beside, s)
    project(1, below)
    for q in (0, 2):
        wait_piece(across, q)
        relay(across, q, pair)
        relay_sibling(across, q)
    forward_wo(0)
    project(2, above)
    for u in (x_below, x_above):
        wait_piece(u, 0)
        relay_sibling(u, 0)
    forward_wo(1)
    project(3, beside)
    for q in (1, 3):
        wait_piece(across, q)
        relay(across, q, pair)
        relay_sibling(across, q)
    for q in (0, 2):
        wait_piece(x_across, q)
        relay_sibling(x_across, q)
    for u in (x_below, x_above):
        wait_piece(u, 1)
        relay_sibling(u, 1)
    project(4, across)
    forward_wo(2)
    for u in (x_below, x_above):
        wait_piece(u, 2)
        relay_sibling(u, 2)
    for q in (1, 3):
        wait_piece(x_across, q)
        relay_sibling(x_across, q)
    make_pairs([5], [x_across])
    for u in (x_below, x_above):
        wait_piece(u, 3)
        relay_sibling(u, 3)
    make_pairs([6, 7], [x_below, x_above])

    made_here = [
        jnp.logical_and(y == 0, x == 0),
        jnp.logical_and(y == 3, x == 1),
    ]
    order = ((0, 0), (3, 0), (1, 0), (0, 1), (2, 0), (2, 1), (3, 1), (1, 1))

    def source_unit(kind, step):
        dy, dx = order[step]
        return ((kind * 2 + y // 2 + dy) % NY) * 2 + (y % 2 + dx) % 2

    def wait_made(kind, step):
        u = source_unit(kind, step)
        part = kv.at[kind, plane_rows(u, c), :]

        @pl.when(jnp.logical_not(made_here[kind]))
        def _():
            arrived(part, kvss.at[0], kvr.at[kind * 8 + u], sibling)

        return part, u

    def forward_made(step):
        for kind in range(2):
            part, u = wait_made(kind, step)
            send(part, part, kvds.at[kind * LATE + step], kvd.at[kind * 8 + u], sibling)

    wait_sibling(x_across)
    make_query([x_across])
    forward_wo(3)
    for step in range(3):
        forward_made(step)
    wait_sibling(x_below)
    wait_sibling(x_above)
    make_query([x_below, x_above])
    for step in range(3, LATE):
        forward_made(step)

    for step in range(LATE, 8):
        for kind in range(2):
            wait_made(kind, step)
    for u in range(8):
        for kind in range(2):
            arrived(kv.at[kind, plane_rows(u, other_c), :], kvds.at[0], kvd.at[kind * 8 + u], sibling)

    scale = HD ** (-0.5)
    my_cols = pl.ds(mult(slot * QCOLS, QCOLS), QCOLS)
    beyond = ((1, 0), (1, 1), (0, 1))

    def theirs(dx, dc):
        return ((x + dx) % 2) * 2 + (c + dc) % 2

    def attend(k):
        b = (y + (2, 1, 3, 0)[k]) % NY
        block = pl.ds(mult(b * 256, 256), 256)
        row = lax.broadcasted_iota(jnp.int32, (256, SEQ), 0) + b * 256
        col = lax.broadcasted_iota(jnp.int32, (256, SEQ), 1)
        for h in range(2):
            cols = slice(h * HD, (h + 1) * HD)
            scores = lax.dot_general(qb[block, cols], kv[0], contract_last, preferred_element_type=F32)
            scores = jnp.where(row >= col, scores, -1e30)
            top = jnp.max(scores, axis=-1, keepdims=True)
            weight = jnp.exp((scores - top) * scale)
            total = jnp.sum(weight, axis=-1, keepdims=True)
            mixed = jnp.dot(weight.astype(BF16), kv[1], preferred_element_type=F32)
            ctx[block, cols] = (mixed / total).astype(BF16)
        target = pl.ds(k * ROWS, ROWS)
        ctx4[target, my_cols] = ctx[pl.ds(mult(b * 256 + slot * ROWS, ROWS), ROWS), :]
        for i, (dx, dc) in enumerate(beyond):
            send(
                ctx.at[pl.ds(mult(b * 256 + theirs(dx, dc) * ROWS, ROWS), ROWS), :],
                ctx4.at[target, my_cols],
                cxs.at[i * 4 + k], cxr.at[i * 4 + k], at(dx=dx, dc=dc),
            )

    def gathered(k):
        for i, (dx, dc) in enumerate(beyond):
            cols = pl.ds(mult(theirs(dx, dc) * QCOLS, QCOLS), QCOLS)
            arrived(
                ctx4.at[k * ROWS:(k + 1) * ROWS, cols], cxs.at[0], cxr.at[i * 4 + k], at(dx=dx, dc=dc)
            )

    stages = [
        ("tensor_0", 4, y, cy, 0),
        ("dp_0", 8, z, cz, 3),
        ("dp_1", 2, xh, chh, 10),
        ("tensor_1", 2, x, cxl, 11),
        ("tensor_2", 2, c, cc, 12),
    ]

    def stage_start(i):
        axis, size, index, buf, first_sem = stages[i]
        for d in range(1, size):
            ssem, rsem = cds.at[first_sem + d - 1], cdr.at[first_sem + d - 1]
            send(buf.at[index], buf.at[index], ssem, rsem, {axis: (index + d) % size})

    def stage_end(i):
        axis, size, index, buf, first_sem = stages[i]
        for d in range(1, size):
            ssem, rsem = cds.at[first_sem + d - 1], cdr.at[first_sem + d - 1]
            source = (index + size - d) % size
            arrived(buf.at[source], ssem, rsem, {axis: source})
        total = buf[0]
        for k in range(1, size):
            total = total + buf[k]
        if i + 1 < len(stages):
            stages[i + 1][3][stages[i + 1][2]] = total
        else:
            total = total * (1.0 / 128.0)
            for j in range(CHUNKS):
                check[0:1, j * CW:(j + 1) * CW] = total[j:j + 1, :]

    attend(0)
    forward_wo(4)
    attend(1)
    forward_wo(5)
    forward_wo(NEAR_CHUNK)
    attend(2)
    attend(3)

    summary = jnp.dot(split3(weights[0:1, :]), ctx[...], preferred_element_type=F32)
    summary = split3(jnp.sum(summary, axis=0, keepdims=True))
    for j in range(CHUNKS):
        term = jnp.dot(summary, wo4[j, my_cols, :], preferred_element_type=F32)
        cy[y, j:j + 1, :] = jnp.sum(term, axis=0, keepdims=True)
    stage_start(0)
    gathered(0)

    far_rows, up_rows, down_rows, own_rows = (slice(k * ROWS, (k + 1) * ROWS) for k in range(4))
    for j in range(CHUNKS):
        if j == 4:
            forward_wo(6)
        arrived(wo_piece(j, sibling_slot), wods.at[0], wod.at[j], sibling)
        arrived(wo_piece(j, far_sibling_slot), wods.at[0], wod.at[8 + j], sibling)
        product = jnp.dot(ctx4[far_rows, :], wo4[j], preferred_element_type=F32)
        pbuf[j, far_rows, :] = product.astype(BF16)
        send(pbuf.at[j, far_rows, :], ra.at[j], ras.at[j], rar.at[j], down if j % 2 else up)

    stage_end(0)
    stage_start(1)
    for k in range(1, 4):
        gathered(k)
    stage_end(1)
    stage_start(2)
    for j in range(CHUNKS):
        product = jnp.dot(ctx4[ROWS:256, :], wo4[j], preferred_element_type=F32)
        pbuf[j, ROWS:256, :] = product.astype(BF16)
        if j % 2 == 0:
            send(pbuf.at[j, down_rows, :], rfa.at[j], rts.at[j], rtr.at[j], down)
        else:
            send(pbuf.at[j, up_rows, :], rfb.at[j], rbs.at[j], rbr.at[j], up)

    for j in range(CHUNKS):
        rows = up_rows if j % 2 == 0 else down_rows
        arrived(ra.at[j], ras.at[j], rar.at[j], sibling)
        pbuf[j, rows, :] = (pbuf[j, rows, :].astype(F32) + ra[j].astype(F32)).astype(BF16)
        if j % 2 == 0:
            send(pbuf.at[j, rows, :], rfb.at[j], rbs.at[j], rbr.at[j], up)
        else:
            send(pbuf.at[j, rows, :], rfa.at[j], rts.at[j], rtr.at[j], down)
    for i in range(2, 4):
        stage_end(i)
        stage_start(i + 1)
    stage_end(4)

    stores = []
    for j in (1, 3, 5, 7, 0, 2, 4, 6):
        arrived(rfb.at[j], rbs.at[j], rbr.at[j], sibling)
        arrived(rfa.at[j], rts.at[j], rtr.at[j], sibling)
        total = pbuf[j, own_rows, :].astype(F32) + rfb[j].astype(F32) + rfa[j].astype(F32)
        cols = slice(j * CW, (j + 1) * CW)
        outv[:, cols] = total.astype(BF16)
        store = pltpu.make_async_copy(outv.at[:, cols], out.at[:, cols], ost.at[j])
        store.start()
        stores.append(store)

    for store in stores:
        store.wait()
    for copy in pending:
        copy.wait_send()
    for copy in local_sends:
        @pl.when(jnp.logical_not(local_user))
        def _():
            copy.wait_send()


def tables():
    half = HD // 2
    inverse = THETA ** (-(np.arange(half, dtype=np.float64) * 2.0 / HD))
    angles = np.arange(SEQ, dtype=np.float64)[:, None] * inverse[None, :]
    cosine, sine = np.cos(angles), np.sin(angles)
    return (
        np.concatenate([cosine, cosine], axis=1).astype(np.float32),
        np.concatenate([-sine, sine], axis=1).astype(np.float32),
    )


def local(tokens, gain, wq, bq, wkv, bkv, wo, check_weights):
    cosine, sine = tables()
    dma = pltpu.SemaphoreType.DMA
    vmem = pltpu.VMEM
    anywhere = pl.BlockSpec(memory_space=pl.ANY)
    inside = pl.BlockSpec(memory_space=pltpu.VMEM)
    attended, total = pl.pallas_call(
        kernel,
        out_shape=(
            jax.ShapeDtypeStruct((ROWS, D), BF16),
            jax.ShapeDtypeStruct((1, D), F32),
        ),
        in_specs=[anywhere, inside, inside, inside, anywhere, anywhere, anywhere, inside, anywhere, anywhere],
        out_specs=(anywhere, inside),
        scratch_shapes=[
            vmem((ROWS, D), BF16),
            vmem((SEQ, D), BF16),
            vmem((D, QCOLS), BF16),
            vmem((128, D), BF16),
            vmem((8, 128), F32),
            vmem((8, 128), F32),
            vmem((SEQ, HD), F32),
            vmem((SEQ, HD), F32),
            vmem((SEQ, QCOLS), BF16),
            vmem((8, ROWS, HD), BF16),
            vmem((2, SEQ, HD), BF16),
            vmem((SEQ, QCOLS), BF16),
            vmem((256, SEQ), BF16),
            vmem((CHUNKS, SEQ, CW), BF16),
            vmem((CHUNKS, 256, CW), BF16),
            vmem((CHUNKS, ROWS, CW), BF16),
            vmem((CHUNKS, ROWS, CW), BF16),
            vmem((CHUNKS, ROWS, CW), BF16),
            vmem((ROWS, D), BF16),
            vmem((8, CHUNKS, CW), F32),
            vmem((2, CHUNKS, CW), F32),
            vmem((2, CHUNKS, CW), F32),
            vmem((2, CHUNKS, CW), F32),
            vmem((4, CHUNKS, CW), F32),
            dma((5,)), dma((4,)), dma((8,)), dma((32,)), dma((32,)), dma((28,)), dma((32,)),
            dma((2,)), dma((2,)), dma((8,)), dma((8,)), dma((16,)), dma((16,)),
            dma((16,)), dma((16,)), dma((22,)), dma((10,)), dma((12,)), dma((12,)),
            dma((8,)), dma((8,)), dma((8,)), dma((8,)), dma((8,)), dma((8,)), dma((8,)),
            dma((13,)), dma((13,)),
        ],
        compiler_params=pltpu.CompilerParams(
            collective_id=0, has_side_effects=True, vmem_limit_bytes=56 * 1024 * 1024
        ),
        name="sublayer",
    )(tokens[0], gain, bq, bkv, wq, wkv.T, wo, check_weights, cosine, sine)
    return attended[None], total.reshape(D)


def solution(mesh):
    torus = Mesh(
        mesh.devices.reshape(8, 2, 4, 2, 2), ("dp_0", "dp_1", "tensor_0", "tensor_1", "tensor_2")
    )
    return jax.shard_map(
        local,
        mesh=torus,
        in_specs=(
            P(DP, TENSOR, None),
            P(),
            P(None, TENSOR),
            P(TENSOR),
            P(None, TENSOR),
            P(TENSOR),
            P(TENSOR, None),
            P(DP, None),
        ),
        out_specs=(P(DP, TENSOR, None), P()),
        check_vma=False,
    )
```

```python
import jax
import jax.numpy as jnp
import numpy as np
from jax import lax
from jax.experimental import pallas as pl
from jax.experimental.pallas import tpu as pltpu
from jax.sharding import Mesh
from jax.sharding import PartitionSpec as P

HD = 128
EPS = 1e-06
THETA = 1000000.0
TENSOR = ("tensor_0", "tensor_1", "tensor_2")
DP = ("dp_0", "dp_1")
MESH = pl.DeviceIdType.MESH
F32 = jnp.float32
BF16 = jnp.bfloat16

NY = 4
NZ = 8
D = 4096
ROWS = 64
QUARTER = 16
QCOLS = 256
SEQ = 1024
CHUNKS = 8
CW = D // CHUNKS
NEAR_CHUNK = 7
LATE = 5
(
    GATHER, SIBLING, SIBLING_WK, SIBLING_BIAS, WO, WO_SIBLING, MADE, MADE_HERE, MADE_SIBLING, CONTEXT, SUM, CHECK,
) = range(12)


def mult(value, by):
    return pl.multiple_of(value, by)


def split3(value):
    hi = value.astype(BF16).astype(F32)
    rest = value - hi
    mid = rest.astype(BF16).astype(F32)
    low = (rest - mid).astype(BF16).astype(F32)
    row = lax.broadcasted_iota(jnp.int32, (16, value.shape[1]), 0)
    rows = jnp.where(row == 0, hi, jnp.where(row == 1, mid, jnp.where(row == 2, low, 0.0)))
    return rows.astype(BF16)


def kernel(
    tokens, gain_in, bq_in, bkv_in, wq, wkv, wo, weights, cos, sin,
    out, check,
    tok, gain_v, bq_v, bkv_v, weights_v, check_v, xg, wqv, wkfull, bmine, bpair, cosv, sinv, qb, kvs, kv,
    ctx, ctx4, wo4, pbuf, ra, rfb, rfa, outv, cy, cz, cc,
    ld, agr, agd, wkr, wor, wod, kvr, kvd, cxr, rar, rbr, rtr, cdr, sent, stored, chain,
):
    z = lax.axis_index("dp_0")
    xh = lax.axis_index("dp_1")
    y = lax.axis_index("tensor_0")
    x = lax.axis_index("tensor_1")
    c = lax.axis_index("tensor_2")
    slot = x * 2 + c
    other_x = (x + 1) % 2
    other_c = (c + 1) % 2

    def at(dy=0, dx=0, dc=0):
        return {"tensor_0": (y + dy) % NY, "tensor_1": (x + dx) % 2, "tensor_2": (c + dc) % 2}

    def unit(dy, dx):
        return ((y + dy) % NY) * 2 + (x + dx) % 2

    up, down, pair, sibling = at(dy=1), at(dy=3), at(dx=1), at(dc=1)
    far = {"dp_1": (xh + 1) % 2, "tensor_1": other_x}

    barrier = pltpu.get_barrier_semaphore()
    peers = [at(dy=dy, dx=dx) for dy in range(4) for dx in range(2) if dy or dx]
    peers += [sibling, at(dx=1, dc=1), far]

    def greet(sem_up, sem_down, distance):
        @pl.when(z + distance < NZ)
        def _():
            pl.semaphore_signal(sem_up, inc=1, device_id={"dp_0": (z + distance) % NZ}, device_id_type=MESH)

        @pl.when(z >= distance)
        def _():
            pl.semaphore_signal(sem_down, inc=1, device_id={"dp_0": (z + NZ - distance) % NZ}, device_id_type=MESH)

    def greet_round(r):
        greet(chain.at[2 * r], chain.at[2 * r + 1], 2 ** r)

    def greeted_round(r):
        distance = 2 ** r

        @pl.when(z >= distance)
        def _():
            pl.semaphore_wait(chain.at[2 * r], 1)

        @pl.when(z + distance < NZ)
        def _():
            pl.semaphore_wait(chain.at[2 * r + 1], 1)

    for peer in peers:
        pl.semaphore_signal(barrier, inc=1, device_id=peer, device_id_type=MESH)
    greet(barrier, barrier, 1)

    contract_last = (((1,), (1,)), ((), ()))
    loads = {}

    def load(name, src, dst, sem):
        loads[name] = pltpu.make_async_copy(src, dst, sem)
        loads[name].start()

    my_wk = wkfull.at[pl.ds(mult(c * 64, 64), 64), :]
    for k, (name, src, dst) in enumerate((
        ("tok", tokens, tok), ("gain", gain_in, gain_v), ("bkv", bkv_in, bkv_v), ("wk", wkv, my_wk),
        ("bq", bq_in, bq_v), ("weights", weights, weights_v), ("wq", wq, wqv), ("cos", cos, cosv), ("sin", sin, sinv),
    )):
        load(name, src, dst, ld.at[k])
    my_wo = pl.ds(mult(slot * QCOLS, QCOLS), QCOLS)
    for j in range(CHUNKS):
        pltpu.make_async_copy(wo.at[:, pl.ds(j * CW, CW)], wo4.at[j, my_wo, :], ld.at[9]).start()

    def send(src, dst, group, rsem, device):
        copy = pltpu.make_async_remote_copy(
            src_ref=src, dst_ref=dst, send_sem=sent.at[group], recv_sem=rsem,
            device_id=device, device_id_type=MESH,
        )
        copy.start()

    def all_sent(group, size):
        pltpu.make_async_remote_copy(
            src_ref=size, dst_ref=size, send_sem=sent.at[group], recv_sem=agr.at[0],
            device_id=sibling, device_id_type=MESH,
        ).wait_send()

    def arrived(dst, rsem):
        pltpu.make_async_remote_copy(
            src_ref=dst, dst_ref=dst, send_sem=sent.at[0], recv_sem=rsem,
            device_id=sibling, device_id_type=MESH,
        ).wait_recv()

    base = (y * 4 + slot) * ROWS
    loads["tok"].wait()
    loads["gain"].wait()
    gain = gain_v[...].astype(F32).reshape(1, D)
    for q in range(4):
        part = tok[q * QUARTER:(q + 1) * QUARTER, :].astype(F32)
        mean = jnp.mean(part * part, axis=-1, keepdims=True)
        xg[pl.ds(mult(base + q * QUARTER, QUARTER), QUARTER), :] = (
            part * lax.rsqrt(mean + EPS) * gain
        ).astype(BF16)

    pl.semaphore_wait(barrier, len(peers) + (z + NZ - 1) // NZ + (2 * NZ - 2 - z) // NZ)
    greet_round(0)

    def piece(u, q):
        return xg.at[pl.ds(mult(u * 128 + c * ROWS + q * QUARTER, QUARTER), QUARTER), :]

    def sibling_piece(u, q):
        return xg.at[pl.ds(mult(u * 128 + other_c * ROWS + q * QUARTER, QUARTER), QUARTER), :]

    def relay(u, q, device):
        send(piece(u, q), piece(u, q), GATHER, agr.at[u * 4 + q], device)

    def relay_sibling(u, q):
        send(piece(u, q), piece(u, q), SIBLING, agd.at[u], sibling)

    def wait_piece(u, q):
        arrived(piece(u, q), agr.at[u * 4 + q])

    def wait_sibling(u):
        arrived(xg.at[plane_rows(u, other_c), :], agd.at[u])

    def plane_rows(u, plane):
        return pl.ds(mult(u * 128 + plane * ROWS, ROWS), ROWS)

    own = unit(0, 0)
    for s in range(4):
        relay(own, s, up)
        relay(own, (s + 2) % 4, down)
        relay(own, s, pair)
    for q in range(4):
        relay_sibling(own, q)

    loads["wk"].wait()
    send(my_wk, my_wk, SIBLING_WK, wkr.at[0], sibling)
    loads["bkv"].wait()
    bias_mine = bkv_v[...].astype(F32).reshape(1, 64)
    bias_mine = jnp.concatenate([bias_mine, bias_mine], axis=1)
    bmine[...] = jnp.broadcast_to(bias_mine, (8, 128))
    send(bmine, bpair, SIBLING_BIAS, wkr.at[1], sibling)

    def wo_piece(j, owner):
        return wo4.at[j, pl.ds(mult(owner * QCOLS, QCOLS), QCOLS), :]

    pltpu.make_async_copy(wo4.at[:, my_wo, :], wo4.at[:, my_wo, :], ld.at[9]).wait()
    for j in range(CHUNKS):
        route = pair if j == NEAR_CHUNK else far
        send(wo_piece(j, slot), wo_piece(j, slot), WO, wor.at[j], route)
        send(wo_piece(j, slot), wo_piece(j, slot), WO_SIBLING, wod.at[CHUNKS], sibling)

    far_slot = other_x * 2 + c
    sibling_slot = x * 2 + other_c
    far_sibling_slot = other_x * 2 + other_c

    def forward_wo(j):
        arrived(wo_piece(j, far_slot), wor.at[j])
        send(wo_piece(j, far_slot), wo_piece(j, far_slot), WO_SIBLING, wod.at[j], sibling)

    arrived(wkfull.at[pl.ds(mult(other_c * 64, 64), 64), :], wkr.at[0])
    arrived(bpair, wkr.at[1])
    first = c == 0
    lane = lax.broadcasted_iota(jnp.int32, (1, 128), 1)
    bias_theirs = bpair[0:1, :]
    low_half = lane < 64
    kv_bias = jnp.where(
        first,
        jnp.where(low_half, bias_mine, bias_theirs),
        jnp.where(low_half, bias_theirs, bias_mine),
    )
    loads["bq"].wait()
    q_bias = bq_v[...].astype(F32).reshape(1, QCOLS)
    loads["wq"].wait()
    loads["cos"].wait()
    loads["sin"].wait()

    chip = y * 2 + x
    is_value = y // 2
    turned = (1 - is_value).astype(F32)
    straight = is_value.astype(F32)
    group = chip % NY
    local_user = group == y

    def rope(value, cosine, sine):
        return value * cosine + pltpu.roll(value, 64, 1) * sine

    def push(step, rows_kv, group, sem, device):
        return pltpu.make_async_remote_copy(
            src_ref=kvs.at[step], dst_ref=kv.at[is_value, rows_kv, :],
            send_sem=sent.at[group], recv_sem=sem, device_id=device, device_id_type=MESH,
        )

    def make_pairs(steps, units):
        lhs = [xg[plane_rows(u, c), :] for u in units]
        lhs = lhs[0] if len(lhs) == 1 else jnp.concatenate(lhs, axis=0)
        made_rows = lax.dot_general(
            lhs, wkfull[...], contract_last, preferred_element_type=F32
        ) + kv_bias
        made_rows = made_rows.astype(BF16).astype(F32)
        for i, (step, u) in enumerate(zip(steps, units)):
            rows_kv = plane_rows(u, c)
            cosine = cosv[rows_kv, :] * turned + straight
            sine = sinv[rows_kv, :] * turned
            result = rope(made_rows[i * ROWS:(i + 1) * ROWS, :], cosine, sine).astype(BF16)
            kvs[step] = result
            late = step >= LATE
            sem = kvr.at[is_value + (2 if late else 0)]

            @pl.when(local_user)
            def _():
                kv[is_value, rows_kv, :] = result

            @pl.when(jnp.logical_not(local_user))
            def _():
                push(step, rows_kv, MADE_HERE, sem, {"tensor_0": group}).start()

            push(step, rows_kv, MADE, sem, {"tensor_0": group, "tensor_1": other_x}).start()
            if late:
                for px in (other_x, x):
                    push(
                        step, rows_kv, MADE, kvd, {"tensor_0": group, "tensor_1": px, "tensor_2": other_c}
                    ).start()

    def make_query(units):
        lhs = [xg[pl.ds(mult(u * 128, 128), 128), :] for u in units]
        lhs = lhs[0] if len(lhs) == 1 else jnp.concatenate(lhs, axis=0)
        query = jnp.dot(lhs, wqv[...], preferred_element_type=F32) + q_bias
        for i, u in enumerate(units):
            rows = pl.ds(mult(u * 128, 128), 128)
            for h in range(2):
                cols = slice(h * HD, (h + 1) * HD)
                part = query[i * 128:(i + 1) * 128, cols]
                qb[rows, cols] = rope(part, cosv[rows, :], sinv[rows, :]).astype(BF16)

    def project(step, u):
        wait_sibling(u)
        make_pairs([step], [u])
        make_query([u])

    below, above, beside, across = unit(3, 0), unit(1, 0), unit(0, 1), unit(2, 0)
    x_across, x_below, x_above = unit(2, 1), unit(3, 1), unit(1, 1)

    greeted_round(0)
    greet_round(1)
    project(0, own)
    for s in range(4):
        wait_piece(below, s)
        if s < 2:
            relay(below, s, up)
        r = (s + 2) % 4
        wait_piece(above, r)
        if s < 2:
            relay(above, r, down)
        wait_piece(beside, s)
        relay(beside, s, up)
        relay(beside, s, down)
        relay_sibling(below, s)
        relay_sibling(above, r)
        relay_sibling(beside, s)
    greeted_round(1)
    greet_round(2)
    project(1, below)
    for q in (0, 2):
        wait_piece(across, q)
        relay(across, q, pair)
        relay_sibling(across, q)
    forward_wo(0)
    project(2, above)
    for u in (x_below, x_above):
        wait_piece(u, 0)
        relay_sibling(u, 0)
    forward_wo(1)
    project(3, beside)
    for q in (1, 3):
        wait_piece(across, q)
        relay(across, q, pair)
        relay_sibling(across, q)
    for q in (0, 2):
        wait_piece(x_across, q)
        relay_sibling(x_across, q)
    for u in (x_below, x_above):
        wait_piece(u, 1)
        relay_sibling(u, 1)
    greeted_round(2)
    project(4, across)
    forward_wo(2)
    for u in (x_below, x_above):
        wait_piece(u, 2)
        relay_sibling(u, 2)
    for q in (1, 3):
        wait_piece(x_across, q)
        relay_sibling(x_across, q)
    make_pairs([5], [x_across])
    for u in (x_below, x_above):
        wait_piece(u, 3)
        relay_sibling(u, 3)
    make_pairs([6, 7], [x_below, x_above])

    made_here = [
        jnp.logical_and(y == 0, x == 0),
        jnp.logical_and(y == 3, x == 1),
    ]
    order = ((0, 0), (3, 0), (1, 0), (0, 1), (2, 0), (2, 1), (3, 1), (1, 1))

    def source_unit(kind, step):
        dy, dx = order[step]
        return ((kind * 2 + y // 2 + dy) % NY) * 2 + (y % 2 + dx) % 2

    def wait_made(kind, steps, late):
        @pl.when(jnp.logical_not(made_here[kind]))
        def _():
            arrived(kv.at[kind, 0:steps * ROWS, :], kvr.at[kind + 2 * late])

    def forward_made(kind):
        wait_made(kind, LATE, 0)
        for step in range(LATE):
            part = kv.at[kind, plane_rows(source_unit(kind, step), c), :]
            send(part, part, MADE_SIBLING, kvd, sibling)

    wait_sibling(x_across)
    make_query([x_across])
    forward_wo(3)
    wait_sibling(x_below)
    wait_sibling(x_above)
    make_query([x_below, x_above])
    for kind in range(2):
        forward_made(kind)
    for kind in range(2):
        wait_made(kind, 8 - LATE, 1)
    arrived(kv.at[0], kvd)

    scale = HD ** (-0.5)
    my_cols = pl.ds(mult(slot * QCOLS, QCOLS), QCOLS)
    beyond = ((1, 0), (1, 1), (0, 1))

    def theirs(dx, dc):
        return ((x + dx) % 2) * 2 + (c + dc) % 2

    def block_attention(v):
        block, before = slice(v * 256, (v + 1) * 256), slice(0, v * 256)
        row = lax.broadcasted_iota(jnp.int32, (256, 256), 0)
        col = lax.broadcasted_iota(jnp.int32, (256, 256), 1)
        for h in range(2):
            cols = slice(h * HD, (h + 1) * HD)
            query = qb[block, cols]
            diagonal = lax.dot_general(query, kv[0, block, :], contract_last, preferred_element_type=F32)
            diagonal = jnp.where(row >= col, diagonal, -1e30)
            top = jnp.max(diagonal, axis=-1, keepdims=True)
            if v:
                earlier = lax.dot_general(query, kv[0, before, :], contract_last, preferred_element_type=F32)
                top = jnp.maximum(top, jnp.max(earlier, axis=-1, keepdims=True))
            weight = jnp.exp((diagonal - top) * scale)
            total = jnp.sum(weight, axis=-1, keepdims=True)
            mixed = jnp.dot(weight.astype(BF16), kv[1, block, :], preferred_element_type=F32)
            if v:
                weight = jnp.exp((earlier - top) * scale)
                total += jnp.sum(weight, axis=-1, keepdims=True)
                mixed += jnp.dot(weight.astype(BF16), kv[1, before, :], preferred_element_type=F32)
            ctx[block, cols] = (mixed / total).astype(BF16)

    def attend(k):
        b = (y + (2, 1, 3, 0)[k]) % NY
        for v in range(NY):
            @pl.when(b == v)
            def _(v=v):
                block_attention(v)

        target = pl.ds(k * ROWS, ROWS)
        ctx4[target, my_cols] = ctx[pl.ds(mult(b * 256 + slot * ROWS, ROWS), ROWS), :]
        for i, (dx, dc) in enumerate(beyond):
            send(
                ctx.at[pl.ds(mult(b * 256 + theirs(dx, dc) * ROWS, ROWS), ROWS), :],
                ctx4.at[target, my_cols],
                CONTEXT, cxr.at[k], at(dx=dx, dc=dc),
            )

    def gathered(k):
        arrived(ctx.at[0:3 * ROWS, :], cxr.at[k])

    def line(axis, index, size):
        return [{axis: (index + d) % size} for d in range(1, size)]

    cross = [
        {"dp_1": (xh + dh) % 2, "tensor_1": (x + dx) % 2, "tensor_2": (c + dc) % 2}
        for dh in range(2) for dx in range(2) for dc in range(2) if dh or dx or dc
    ]
    stages = [
        (line("tensor_0", y, NY), cy, y),
        (line("dp_0", z, NZ), cz, z),
        (cross, cc, xh * 4 + slot),
    ]

    def stage_start(i):
        devices, buf, index = stages[i]
        for device in devices:
            send(buf.at[index], buf.at[index], CHECK, cdr.at[i], device)

    def stage_end(i):
        devices, buf, _ = stages[i]
        arrived(buf.at[0:len(devices)], cdr.at[i])
        total = buf[0]
        for k in range(1, len(devices) + 1):
            total = total + buf[k]
        if i + 1 < len(stages):
            stages[i + 1][1][stages[i + 1][2]] = total
        else:
            total = total * (1.0 / 128.0)
            for j in range(CHUNKS):
                check_v[0:1, j * CW:(j + 1) * CW] = total[j:j + 1, :]
            pltpu.make_async_copy(check_v, check, stored.at[1]).start()

    attend(0)
    forward_wo(4)
    attend(1)
    forward_wo(5)
    forward_wo(NEAR_CHUNK)
    attend(2)
    attend(3)

    loads["weights"].wait()
    summary = jnp.dot(split3(weights_v[...]), ctx[...], preferred_element_type=F32)
    summary = split3(jnp.sum(summary, axis=0, keepdims=True))
    for j in range(CHUNKS):
        term = jnp.dot(summary, wo4[j, my_cols, :], preferred_element_type=F32)
        cy[y, j:j + 1, :] = jnp.sum(term, axis=0, keepdims=True)
    stage_start(0)
    gathered(0)

    far_rows, up_rows, down_rows, own_rows = (slice(k * ROWS, (k + 1) * ROWS) for k in range(4))
    arrived(wo4.at[:, pl.ds(mult(sibling_slot * QCOLS, QCOLS), QCOLS), :], wod.at[CHUNKS])
    for j in range(CHUNKS):
        if j == 4:
            forward_wo(6)
        arrived(wo_piece(j, far_sibling_slot), wod.at[j])
        product = jnp.dot(ctx4[far_rows, :], wo4[j], preferred_element_type=F32)
        pbuf[j, far_rows, :] = product.astype(BF16)
        send(pbuf.at[j, far_rows, :], ra.at[j], SUM, rar.at[j], down if j % 2 else up)

    stage_end(0)
    stage_start(1)
    for k in range(1, 4):
        gathered(k)
    for j in range(CHUNKS):
        product = jnp.dot(ctx4[ROWS:256, :], wo4[j], preferred_element_type=F32)
        pbuf[j, ROWS:256, :] = product.astype(BF16)
        if j % 2 == 0:
            send(pbuf.at[j, down_rows, :], rfa.at[j], SUM, rtr.at[j], down)
        else:
            send(pbuf.at[j, up_rows, :], rfb.at[j], SUM, rbr.at[j], up)

    for j in range(CHUNKS):
        rows = up_rows if j % 2 == 0 else down_rows
        arrived(ra.at[j], rar.at[j])
        pbuf[j, rows, :] = (pbuf[j, rows, :].astype(F32) + ra[j].astype(F32)).astype(BF16)
        if j % 2 == 0:
            send(pbuf.at[j, rows, :], rfb.at[j], SUM, rbr.at[j], up)
        else:
            send(pbuf.at[j, rows, :], rfa.at[j], SUM, rtr.at[j], down)
    stage_end(1)
    stage_start(2)
    stage_end(2)

    for j in (1, 3, 5, 7, 0, 2, 4, 6):
        arrived(rfb.at[j], rbr.at[j])
        arrived(rfa.at[j], rtr.at[j])
        total = pbuf[j, own_rows, :].astype(F32) + rfb[j].astype(F32) + rfa[j].astype(F32)
        cols = slice(j * CW, (j + 1) * CW)
        outv[:, cols] = total.astype(BF16)
        pltpu.make_async_copy(outv.at[:, cols], out.at[:, cols], stored.at[0]).start()

    all_sent(GATHER, xg.at[0:28 * QUARTER, :])
    all_sent(SIBLING, xg.at[0:32 * QUARTER, :])
    all_sent(SIBLING_WK, my_wk)
    all_sent(SIBLING_BIAS, bmine)
    all_sent(WO, wo4.at[:, 0:QCOLS, :])
    all_sent(WO_SIBLING, wo4.at[:, 0:2 * QCOLS, :])
    all_sent(MADE, kv.at[0, 0:14 * ROWS, :])
    all_sent(MADE_SIBLING, kv.at[:, 0:LATE * ROWS, :])
    all_sent(CONTEXT, ctx.at[0:12 * ROWS, :])
    all_sent(SUM, xg.at[0:192, :])
    all_sent(CHECK, wo4.at[0, 0:17 * 16, :])

    @pl.when(jnp.logical_not(local_user))
    def _():
        all_sent(MADE_HERE, kv.at[0, 0:8 * ROWS, :])

    pltpu.make_async_copy(outv, out, stored.at[0]).wait()
    pltpu.make_async_copy(check_v, check, stored.at[1]).wait()


def tables():
    half = HD // 2
    inverse = THETA ** (-(np.arange(half, dtype=np.float64) * 2.0 / HD))
    angles = np.arange(SEQ, dtype=np.float64)[:, None] * inverse[None, :]
    cosine, sine = np.cos(angles), np.sin(angles)
    return (
        np.concatenate([cosine, cosine], axis=1).astype(np.float32),
        np.concatenate([-sine, sine], axis=1).astype(np.float32),
    )


def local(tokens, gain, wq, bq, wkv, bkv, wo, check_weights):
    cosine, sine = tables()
    dma = pltpu.SemaphoreType.DMA
    vmem = pltpu.VMEM
    anywhere = pl.BlockSpec(memory_space=pl.ANY)
    attended, total = pl.pallas_call(
        kernel,
        out_shape=(
            jax.ShapeDtypeStruct((ROWS, D), BF16),
            jax.ShapeDtypeStruct((1, D), F32),
        ),
        in_specs=[anywhere] * 10,
        out_specs=(anywhere, anywhere),
        scratch_shapes=[
            vmem((ROWS, D), BF16),
            vmem((D,), BF16),
            vmem((QCOLS,), BF16),
            vmem((64,), BF16),
            vmem((1, SEQ), F32),
            vmem((1, D), F32),
            vmem((SEQ, D), BF16),
            vmem((D, QCOLS), BF16),
            vmem((128, D), BF16),
            vmem((8, 128), F32),
            vmem((8, 128), F32),
            vmem((SEQ, HD), F32),
            vmem((SEQ, HD), F32),
            vmem((SEQ, QCOLS), BF16),
            vmem((8, ROWS, HD), BF16),
            vmem((2, SEQ, HD), BF16),
            vmem((SEQ, QCOLS), BF16),
            vmem((256, SEQ), BF16),
            vmem((CHUNKS, SEQ, CW), BF16),
            vmem((CHUNKS, 256, CW), BF16),
            vmem((CHUNKS, ROWS, CW), BF16),
            vmem((CHUNKS, ROWS, CW), BF16),
            vmem((CHUNKS, ROWS, CW), BF16),
            vmem((ROWS, D), BF16),
            vmem((NY, CHUNKS, CW), F32),
            vmem((NZ, CHUNKS, CW), F32),
            vmem((8, CHUNKS, CW), F32),
            dma((10,)), dma((32,)), dma((8,)), dma((2,)), dma((CHUNKS,)), dma((CHUNKS + 1,)),
            dma((4,)), dma, dma((4,)), dma((CHUNKS,)), dma((CHUNKS,)), dma((CHUNKS,)),
            dma((3,)), dma((12,)), dma((2,)), pltpu.SemaphoreType.REGULAR((6,)),
        ],
        compiler_params=pltpu.CompilerParams(
            collective_id=0, has_side_effects=True, vmem_limit_bytes=56 * 1024 * 1024
        ),
        name="sublayer",
    )(tokens[0], gain, bq, bkv, wq, wkv.T, wo, check_weights, cosine, sine)
    return attended[None], total.reshape(D)


def solution(mesh):
    torus = Mesh(
        mesh.devices.reshape(8, 2, 4, 2, 2), ("dp_0", "dp_1", "tensor_0", "tensor_1", "tensor_2")
    )
    return jax.shard_map(
        local,
        mesh=torus,
        in_specs=(
            P(DP, TENSOR, None),
            P(),
            P(None, TENSOR),
            P(TENSOR),
            P(None, TENSOR),
            P(TENSOR),
            P(TENSOR, None),
            P(DP, None),
        ),
        out_specs=(P(DP, TENSOR, None), P()),
        check_vma=False,
    )
```

```python
import jax
import jax.numpy as jnp
import numpy as np
from jax import lax
from jax.experimental import pallas as pl
from jax.experimental.pallas import tpu as pltpu
from jax.sharding import Mesh
from jax.sharding import PartitionSpec as P

HD = 128
EPS = 1e-06
THETA = 1000000.0
TENSOR = ("tensor_0", "tensor_1", "tensor_2")
DP = ("dp_0", "dp_1")
MESH = pl.DeviceIdType.MESH
F32 = jnp.float32
BF16 = jnp.bfloat16

NY = 4
NZ = 8
D = 4096
ROWS = 64
QUARTER = 16
QCOLS = 256
SEQ = 1024
CHUNKS = 8
CW = D // CHUNKS
LATE = 4
NEAR_CHUNK = 7
LAST_CHUNK = 6
(
    GATHER, SIBLING, SIBLING_WK, SIBLING_BIAS, WO, WO_SIBLING, MADE, MADE_HERE, MADE_SIBLING, CONTEXT, SUM, CHECK,
) = range(12)


def mult(value, by):
    return pl.multiple_of(value, by)


def split3(value):
    hi = value.astype(BF16).astype(F32)
    rest = value - hi
    mid = rest.astype(BF16).astype(F32)
    low = (rest - mid).astype(BF16).astype(F32)
    row = lax.broadcasted_iota(jnp.int32, (16, value.shape[1]), 0)
    rows = jnp.where(row == 0, hi, jnp.where(row == 1, mid, jnp.where(row == 2, low, 0.0)))
    return rows.astype(BF16)


def kernel(
    tokens, gain_in, bq_in, bkv_in, wq, wkv, wo, weights, cos, sin,
    out, check,
    tok, gain_v, bq_v, bkv_v, weights_v, xg, wqv, wkfull, wkt, bmine, bpair, cosv, sinv, qb, kvs, kv,
    ctx, ctx4, wo4, pbuf, ra, rfb, rfa, cy, cz, cc,
    ld, agr, agx, agd, wkr, wor, wod, kvr, kvd, cxr, rar, rbr, rtr, cdr, sent, chain,
):
    z = lax.axis_index("dp_0")
    xh = lax.axis_index("dp_1")
    y = lax.axis_index("tensor_0")
    x = lax.axis_index("tensor_1")
    c = lax.axis_index("tensor_2")
    slot = x * 2 + c
    other_x = (x + 1) % 2
    other_c = (c + 1) % 2

    def at(dy=0, dx=0, dc=0):
        return {"tensor_0": (y + dy) % NY, "tensor_1": (x + dx) % 2, "tensor_2": (c + dc) % 2}

    def unit(dy, dx):
        return ((y + dy) % NY) * 2 + (x + dx) % 2

    up, down, pair, sibling = at(dy=1), at(dy=3), at(dx=1), at(dc=1)
    far = {"dp_1": (xh + 1) % 2, "tensor_1": other_x}

    barrier = pltpu.get_barrier_semaphore()
    peers = [at(dy=dy, dx=dx) for dy in range(4) for dx in range(2) if dy or dx]
    peers += [sibling, at(dx=1, dc=1), far]

    def greet(sem_up, sem_down, distance):
        @pl.when(z + distance < NZ)
        def _():
            pl.semaphore_signal(sem_up, inc=1, device_id={"dp_0": (z + distance) % NZ}, device_id_type=MESH)

        @pl.when(z >= distance)
        def _():
            pl.semaphore_signal(sem_down, inc=1, device_id={"dp_0": (z + NZ - distance) % NZ}, device_id_type=MESH)

    def greet_round(r):
        greet(chain.at[2 * r], chain.at[2 * r + 1], 2 ** r)

    def greeted_round(r):
        distance = 2 ** r

        @pl.when(z >= distance)
        def _():
            pl.semaphore_wait(chain.at[2 * r], 1)

        @pl.when(z + distance < NZ)
        def _():
            pl.semaphore_wait(chain.at[2 * r + 1], 1)

    for peer in peers:
        pl.semaphore_signal(barrier, inc=1, device_id=peer, device_id_type=MESH)
    greet(barrier, barrier, 1)

    contract_last = (((1,), (1,)), ((), ()))
    loads = {}

    def load(name, src, dst, sem):
        loads[name] = pltpu.make_async_copy(src, dst, sem)
        loads[name].start()

    my_wk = wkfull.at[pl.ds(mult(c * 64, 64), 64), :]
    for k, (name, src, dst) in enumerate((
        ("tok", tokens, tok), ("gain", gain_in, gain_v), ("bkv", bkv_in, bkv_v), ("wk", wkv, my_wk),
        ("bq", bq_in, bq_v), ("weights", weights, weights_v), ("wq", wq, wqv), ("cos", cos, cosv), ("sin", sin, sinv),
    )):
        load(name, src, dst, ld.at[k])
    my_wo = pl.ds(mult(slot * QCOLS, QCOLS), QCOLS)
    for j in range(CHUNKS):
        pltpu.make_async_copy(wo.at[:, pl.ds(j * CW, CW)], wo4.at[j, my_wo, :], ld.at[9]).start()

    def send(src, dst, group, rsem, device):
        copy = pltpu.make_async_remote_copy(
            src_ref=src, dst_ref=dst, send_sem=sent.at[group], recv_sem=rsem,
            device_id=device, device_id_type=MESH,
        )
        copy.start()

    def all_sent(group, size):
        pltpu.make_async_remote_copy(
            src_ref=size, dst_ref=size, send_sem=sent.at[group], recv_sem=agr.at[0],
            device_id=sibling, device_id_type=MESH,
        ).wait_send()

    def arrived(dst, rsem):
        pltpu.make_async_remote_copy(
            src_ref=dst, dst_ref=dst, send_sem=sent.at[0], recv_sem=rsem,
            device_id=sibling, device_id_type=MESH,
        ).wait_recv()

    base = (y * 4 + slot) * ROWS
    loads["tok"].wait()
    loads["gain"].wait()
    gain = gain_v[...].astype(F32).reshape(1, D)
    for q in range(4):
        part = tok[q * QUARTER:(q + 1) * QUARTER, :].astype(F32)
        mean = jnp.mean(part * part, axis=-1, keepdims=True)
        xg[pl.ds(mult(base + q * QUARTER, QUARTER), QUARTER), :] = (
            part * lax.rsqrt(mean + EPS) * gain
        ).astype(BF16)

    pl.semaphore_wait(barrier, len(peers) + (z + NZ - 1) // NZ + (2 * NZ - 2 - z) // NZ)
    greet_round(0)

    def piece(u, q):
        return xg.at[pl.ds(mult(u * 128 + c * ROWS + q * QUARTER, QUARTER), QUARTER), :]

    def sibling_piece(u, q):
        return xg.at[pl.ds(mult(u * 128 + other_c * ROWS + q * QUARTER, QUARTER), QUARTER), :]

    def relay(u, q, device):
        send(piece(u, q), piece(u, q), GATHER, agr.at[u * 4 + q], device)

    def relay_sibling(u, q):
        send(piece(u, q), piece(u, q), SIBLING, agd.at[u], sibling)

    def wait_piece(u, q):
        arrived(piece(u, q), agr.at[u * 4 + q])

    def half_piece(u, q, side):
        rows = pl.ds(mult(u * 128 + c * ROWS + q * QUARTER, QUARTER), QUARTER)
        return xg.at[rows, side * (D // 2):(side + 1) * (D // 2)]

    def relay_half(u, q, side, sem, device):
        send(half_piece(u, q, side), half_piece(u, q, side), GATHER, sem, device)

    def wait_sibling(u):
        arrived(xg.at[plane_rows(u, other_c), :], agd.at[u])

    def plane_rows(u, plane):
        return pl.ds(mult(u * 128 + plane * ROWS, ROWS), ROWS)

    own = unit(0, 0)
    for s in range(4):
        if s < 3:
            relay(own, s, up)
            relay(own, (s + 2) % 4, down)
        relay(own, s, pair)
    for q in range(4):
        relay_sibling(own, q)

    loads["wk"].wait()
    send(my_wk, my_wk, SIBLING_WK, wkr.at[0], sibling)
    loads["bkv"].wait()
    bias_mine = bkv_v[...].astype(F32).reshape(1, 64)
    bias_mine = jnp.concatenate([bias_mine, bias_mine], axis=1)
    bmine[...] = jnp.broadcast_to(bias_mine, (8, 128))
    send(bmine, bpair, SIBLING_BIAS, wkr.at[1], sibling)

    def wo_piece(j, owner):
        return wo4.at[j, pl.ds(mult(owner * QCOLS, QCOLS), QCOLS), :]

    pltpu.make_async_copy(wo4.at[:, my_wo, :], wo4.at[:, my_wo, :], ld.at[9]).wait()
    for j in range(CHUNKS):
        if j != NEAR_CHUNK:
            send(wo_piece(j, slot), wo_piece(j, slot), WO, wor.at[j], far)
        send(wo_piece(j, slot), wo_piece(j, slot), WO_SIBLING, wod.at[CHUNKS], sibling)

    def send_near_chunk(half):
        part = wo4.at[NEAR_CHUNK, pl.ds(mult(slot * QCOLS + half * 128, 128), 128), :]
        send(part, part, WO, wor.at[NEAR_CHUNK], pair)

    far_slot = other_x * 2 + c
    sibling_slot = x * 2 + other_c
    far_sibling_slot = other_x * 2 + other_c

    def forward_wo(j):
        arrived(wo_piece(j, far_slot), wor.at[j])
        send(wo_piece(j, far_slot), wo_piece(j, far_slot), WO_SIBLING, wod.at[j], sibling)

    arrived(wkfull.at[pl.ds(mult(other_c * 64, 64), 64), :], wkr.at[0])
    arrived(bpair, wkr.at[1])
    for i in range(8):
        cols = slice(i * 512, (i + 1) * 512)
        wkt[cols, :] = wkfull[:, cols].T
    first = c == 0
    lane = lax.broadcasted_iota(jnp.int32, (1, 128), 1)
    bias_theirs = bpair[0:1, :]
    low_half = lane < 64
    kv_bias = jnp.where(
        first,
        jnp.where(low_half, bias_mine, bias_theirs),
        jnp.where(low_half, bias_theirs, bias_mine),
    )
    loads["bq"].wait()
    q_bias = bq_v[...].astype(F32).reshape(1, QCOLS)
    loads["wq"].wait()
    loads["cos"].wait()
    loads["sin"].wait()

    chip = y * 2 + x
    is_value = y // 2
    turned = (1 - is_value).astype(F32)
    straight = is_value.astype(F32)
    group = chip % NY
    local_user = group == y

    def rope(value, cosine, sine):
        return value * cosine + pltpu.roll(value, 64, 1) * sine

    def push(step, rows_kv, group, sem, device):
        return pltpu.make_async_remote_copy(
            src_ref=kvs.at[step], dst_ref=kv.at[is_value, rows_kv, :],
            send_sem=sent.at[group], recv_sem=sem, device_id=device, device_id_type=MESH,
        )

    def make_pairs(steps, units):
        lhs = [xg[plane_rows(u, c), :] for u in units]
        lhs = lhs[0] if len(lhs) == 1 else jnp.concatenate(lhs, axis=0)
        made_rows = jnp.dot(lhs, wkt[...], preferred_element_type=F32) + kv_bias
        made_rows = made_rows.astype(BF16).astype(F32)
        for i, (step, u) in enumerate(zip(steps, units)):
            rows_kv = plane_rows(u, c)
            cosine = cosv[rows_kv, :] * turned + straight
            sine = sinv[rows_kv, :] * turned
            result = rope(made_rows[i * ROWS:(i + 1) * ROWS, :], cosine, sine).astype(BF16)
            kvs[step] = result
            late = step >= LATE
            sem = kvr.at[is_value + (2 if late else 0)]

            @pl.when(local_user)
            def _():
                kv[is_value, rows_kv, :] = result

            @pl.when(jnp.logical_not(local_user))
            def _():
                push(step, rows_kv, MADE_HERE, sem, {"tensor_0": group}).start()

            push(step, rows_kv, MADE, sem, {"tensor_0": group, "tensor_1": other_x}).start()
            if late:
                for px in (other_x, x):
                    push(
                        step, rows_kv, MADE, kvd, {"tensor_0": group, "tensor_1": px, "tensor_2": other_c}
                    ).start()

    def make_query(units):
        lhs = [xg[pl.ds(mult(u * 128, 128), 128), :] for u in units]
        lhs = lhs[0] if len(lhs) == 1 else jnp.concatenate(lhs, axis=0)
        query = jnp.dot(lhs, wqv[...], preferred_element_type=F32) + q_bias
        for i, u in enumerate(units):
            rows = pl.ds(mult(u * 128, 128), 128)
            for h in range(2):
                cols = slice(h * HD, (h + 1) * HD)
                part = query[i * 128:(i + 1) * 128, cols]
                qb[rows, cols] = rope(part, cosv[rows, :], sinv[rows, :]).astype(BF16)

    def project(step, u):
        wait_sibling(u)
        make_pairs([step], [u])
        make_query([u])

    below, above, beside, across = unit(3, 0), unit(1, 0), unit(0, 1), unit(2, 0)
    x_across, x_below, x_above = unit(2, 1), unit(3, 1), unit(1, 1)

    greeted_round(0)
    greet_round(1)
    project(0, own)
    def relay_across(*quarters):
        for q in quarters:
            wait_piece(across, q)
            relay(across, q, pair)
            relay_sibling(across, q)

    def relay_beside(q):
        for device, halved in ((up, 0), (down, 2)):
            if q == halved:
                relay_half(beside, q, 0, agr.at[beside * 4 + q], device)
            else:
                relay(beside, q, device)

    for s in range(4):
        if s == 3:
            relay_across(0, 2)
        r = (s + 2) % 4
        wait_piece(below, s)
        wait_piece(above, r)
        if s < 2:
            relay(below, s, up)
            relay(above, r, down)
        if s == 0:
            relay(own, 3, up)
            relay(own, 1, down)
            relay_half(below, s, 1, agx.at[0], pair)
            relay_half(above, r, 1, agx.at[1], pair)
        wait_piece(beside, s)
        for q in ((), (0, 1), (2,), (3,))[s]:
            relay_beside(q)
        relay_sibling(below, s)
        relay_sibling(above, r)
        relay_sibling(beside, s)
    greeted_round(1)
    greet_round(2)

    def wait_x_neighbours(q):
        for k, (u, halved) in enumerate(((x_below, 0), (x_above, 2))):
            if q == halved:
                arrived(half_piece(u, q, 0), agr.at[u * 4 + q])
                arrived(half_piece(u, q, 1), agx.at[k])
            else:
                wait_piece(u, q)
            relay_sibling(u, q)

    def wait_x_across(*quarters):
        for q in quarters:
            wait_piece(x_across, q)
            relay_sibling(x_across, q)

    project(1, below)
    relay_across(1, 3)
    send_near_chunk(0)
    project(2, above)
    forward_wo(0)
    project(3, beside)
    wait_x_neighbours(0)
    forward_wo(1)
    wait_x_across(0, 2)
    wait_x_neighbours(1)
    greeted_round(2)
    project(4, across)
    forward_wo(2)
    wait_x_neighbours(2)
    wait_x_across(1, 3)
    make_pairs([5], [x_across])
    wait_x_neighbours(3)
    make_pairs([6, 7], [x_below, x_above])
    send_near_chunk(1)

    made_here = [
        jnp.logical_and(y == 0, x == 0),
        jnp.logical_and(y == 3, x == 1),
    ]
    order = ((0, 0), (3, 0), (1, 0), (0, 1), (2, 0), (2, 1), (3, 1), (1, 1))

    def source_unit(kind, step):
        dy, dx = order[step]
        return ((kind * 2 + y // 2 + dy) % NY) * 2 + (y % 2 + dx) % 2

    def wait_made(kind, steps, late):
        @pl.when(jnp.logical_not(made_here[kind]))
        def _():
            arrived(kv.at[kind, 0:steps * ROWS, :], kvr.at[kind + 2 * late])

    def forward_made(kind):
        wait_made(kind, LATE, 0)
        for step in range(LATE):
            part = kv.at[kind, plane_rows(source_unit(kind, step), c), :]
            send(part, part, MADE_SIBLING, kvd, sibling)

    for kind in range(2):
        forward_made(kind)
    wait_sibling(x_across)
    make_query([x_across])
    forward_wo(3)
    wait_sibling(x_below)
    wait_sibling(x_above)
    make_query([x_below, x_above])
    for kind in range(2):
        wait_made(kind, 8 - LATE, 1)
    arrived(kv.at[0], kvd)

    scale = HD ** (-0.5)
    my_cols = pl.ds(mult(slot * QCOLS, QCOLS), QCOLS)
    beyond = ((1, 0), (1, 1), (0, 1))

    def theirs(dx, dc):
        return ((x + dx) % 2) * 2 + (c + dc) % 2

    def head_attention(v, h):
        block, before = slice(v * 256, (v + 1) * 256), slice(0, v * 256)
        row = lax.broadcasted_iota(jnp.int32, (256, 256), 0)
        col = lax.broadcasted_iota(jnp.int32, (256, 256), 1)
        cols = slice(h * HD, (h + 1) * HD)
        query = qb[block, cols]
        diagonal = lax.dot_general(query, kv[0, block, :], contract_last, preferred_element_type=F32)
        diagonal = jnp.where(row >= col, diagonal, -1e30)
        top = jnp.max(diagonal, axis=-1, keepdims=True)
        if v:
            earlier = lax.dot_general(query, kv[0, before, :], contract_last, preferred_element_type=F32)
            top = jnp.maximum(top, jnp.max(earlier, axis=-1, keepdims=True))
        weight = jnp.exp((diagonal - top) * scale)
        total = jnp.sum(weight, axis=-1, keepdims=True)
        mixed = jnp.dot(weight.astype(BF16), kv[1, block, :], preferred_element_type=F32)
        if v:
            weight = jnp.exp((earlier - top) * scale)
            total += jnp.sum(weight, axis=-1, keepdims=True)
            mixed += jnp.dot(weight.astype(BF16), kv[1, before, :], preferred_element_type=F32)
        ctx[block, cols] = (mixed / total).astype(BF16)

    def attend(k):
        b = (y + (2, 1, 3, 0)[k]) % NY
        target = pl.ds(k * ROWS, ROWS)
        for h in range(2):
            for v in range(NY):
                @pl.when(b == v)
                def _(v=v, h=h):
                    head_attention(v, h)

            cols = slice(h * HD, (h + 1) * HD)
            head = pl.ds(mult(slot * QCOLS + h * HD, HD), HD)
            for dx, dc in beyond:
                send(
                    ctx.at[pl.ds(mult(b * 256 + theirs(dx, dc) * ROWS, ROWS), ROWS), cols],
                    ctx4.at[target, head],
                    CONTEXT, cxr.at[k], at(dx=dx, dc=dc),
                )
        ctx4[target, my_cols] = ctx[pl.ds(mult(b * 256 + slot * ROWS, ROWS), ROWS), :]

    def gathered(k):
        arrived(ctx.at[0:3 * ROWS, :], cxr.at[k])

    def line(axis, index, size):
        return [{axis: (index + d) % size} for d in range(1, size)]

    cross = [
        {"dp_1": (xh + dh) % 2, "tensor_1": (x + dx) % 2, "tensor_2": (c + dc) % 2}
        for dh in range(2) for dx in range(2) for dc in range(2) if dh or dx or dc
    ]
    stages = [
        (line("tensor_0", y, NY), cy, y),
        (line("dp_0", z, NZ), cz, z),
        (cross, cc, xh * 4 + slot),
    ]

    def stage_start(i):
        devices, buf, index = stages[i]
        for device in devices:
            send(buf.at[index], buf.at[index], CHECK, cdr.at[i], device)

    def stage_end(i):
        devices, buf, _ = stages[i]
        arrived(buf.at[0:len(devices)], cdr.at[i])
        total = buf[0]
        for k in range(1, len(devices) + 1):
            total = total + buf[k]
        if i + 1 < len(stages):
            stages[i + 1][1][stages[i + 1][2]] = total
        else:
            total = total * (1.0 / 128.0)
            for j in range(CHUNKS):
                check[0:1, j * CW:(j + 1) * CW] = total[j:j + 1, :]

    attend(0)
    forward_wo(4)
    attend(1)
    forward_wo(5)
    attend(2)
    forward_wo(NEAR_CHUNK)
    attend(3)

    loads["weights"].wait()
    summary = jnp.dot(split3(weights_v[...]), ctx[...], preferred_element_type=F32)
    summary = split3(jnp.sum(summary, axis=0, keepdims=True))
    for j in range(CHUNKS):
        term = jnp.dot(summary, wo4[j, my_cols, :], preferred_element_type=F32)
        cy[y, j:j + 1, :] = jnp.sum(term, axis=0, keepdims=True)
    stage_start(0)
    gathered(0)

    far_rows, up_rows, down_rows, own_rows = (slice(k * ROWS, (k + 1) * ROWS) for k in range(4))
    arrived(wo4.at[:, pl.ds(mult(sibling_slot * QCOLS, QCOLS), QCOLS), :], wod.at[CHUNKS])

    def far_target(j):
        arrived(wo_piece(j, far_sibling_slot), wod.at[j])
        product = jnp.dot(ctx4[far_rows, :], wo4[j], preferred_element_type=F32)
        pbuf[j, far_rows, :] = product.astype(BF16)
        send(pbuf.at[j, far_rows, :], ra.at[j], SUM, rar.at[j], down if j % 2 else up)

    def near_targets(j):
        product = jnp.dot(ctx4[ROWS:256, :], wo4[j], preferred_element_type=F32)
        pbuf[j, ROWS:256, :] = product.astype(BF16)
        if j % 2 == 0:
            send(pbuf.at[j, down_rows, :], rfa.at[j], SUM, rtr.at[j], down)
        else:
            send(pbuf.at[j, up_rows, :], rfb.at[j], SUM, rbr.at[j], up)

    def relay_sum(j):
        rows = up_rows if j % 2 == 0 else down_rows
        arrived(ra.at[j], rar.at[j])
        pbuf[j, rows, :] = (pbuf[j, rows, :].astype(F32) + ra[j].astype(F32)).astype(BF16)
        if j % 2 == 0:
            send(pbuf.at[j, rows, :], rfb.at[j], SUM, rbr.at[j], up)
        else:
            send(pbuf.at[j, rows, :], rfa.at[j], SUM, rtr.at[j], down)

    early = [j for j in range(CHUNKS) if j != LAST_CHUNK]
    for j in early:
        far_target(j)
    forward_wo(LAST_CHUNK)
    for k in range(1, 4):
        gathered(k)
    for j in early:
        near_targets(j)
        if j == 1:
            stage_end(0)
            stage_start(1)
    far_target(LAST_CHUNK)
    near_targets(LAST_CHUNK)
    for j in early + [LAST_CHUNK]:
        relay_sum(j)
    stage_end(1)
    stage_start(2)
    for j in early + [LAST_CHUNK]:
        arrived(rfb.at[j], rbr.at[j])
        arrived(rfa.at[j], rtr.at[j])
        total = pbuf[j, own_rows, :].astype(F32) + rfb[j].astype(F32) + rfa[j].astype(F32)
        cols = slice(j * CW, (j + 1) * CW)
        out[:, cols] = total.astype(BF16)

    stage_end(2)

    all_sent(GATHER, xg.at[0:28 * QUARTER, :])
    all_sent(SIBLING, xg.at[0:32 * QUARTER, :])
    all_sent(SIBLING_WK, my_wk)
    all_sent(SIBLING_BIAS, bmine)
    all_sent(WO, wo4.at[:, 0:QCOLS, :])
    all_sent(WO_SIBLING, wo4.at[:, 0:2 * QCOLS, :])
    all_sent(MADE, kv.at[0, 0:(24 - 2 * LATE) * ROWS, :])
    all_sent(MADE_SIBLING, kv.at[:, 0:LATE * ROWS, :])
    all_sent(CONTEXT, ctx.at[0:12 * ROWS, :])
    all_sent(SUM, xg.at[0:192, :])
    all_sent(CHECK, wo4.at[0, 0:17 * 16, :])

    @pl.when(jnp.logical_not(local_user))
    def _():
        all_sent(MADE_HERE, kv.at[0, 0:8 * ROWS, :])


def store_results(attended, total, out, check, sem):
    copies = (pltpu.make_async_copy(total, check, sem.at[1]), pltpu.make_async_copy(attended, out, sem.at[0]))
    for copy in copies:
        copy.start()
    for copy in copies:
        copy.wait()


def tables():
    half = HD // 2
    inverse = THETA ** (-(np.arange(half, dtype=np.float64) * 2.0 / HD))
    angles = np.arange(SEQ, dtype=np.float64)[:, None] * inverse[None, :]
    cosine, sine = np.cos(angles), np.sin(angles)
    return (
        np.concatenate([cosine, cosine], axis=1).astype(np.float32),
        np.concatenate([-sine, sine], axis=1).astype(np.float32),
    )


def local(tokens, gain, wq, bq, wkv, bkv, wo, check_weights):
    cosine, sine = tables()
    dma = pltpu.SemaphoreType.DMA
    vmem = pltpu.VMEM
    anywhere = pl.BlockSpec(memory_space=pl.ANY)
    inside = pl.BlockSpec(memory_space=pltpu.VMEM)
    attended, total = pl.pallas_call(
        kernel,
        out_shape=(
            pltpu.VMEM((ROWS, D), BF16),
            pltpu.VMEM((1, D), F32),
        ),
        in_specs=[anywhere] * 10,
        out_specs=(inside, inside),
        scratch_shapes=[
            vmem((ROWS, D), BF16),
            vmem((D,), BF16),
            vmem((QCOLS,), BF16),
            vmem((64,), BF16),
            vmem((1, SEQ), F32),
            vmem((SEQ, D), BF16),
            vmem((D, QCOLS), BF16),
            vmem((128, D), BF16),
            vmem((D, 128), BF16),
            vmem((8, 128), F32),
            vmem((8, 128), F32),
            vmem((SEQ, HD), F32),
            vmem((SEQ, HD), F32),
            vmem((SEQ, QCOLS), BF16),
            vmem((8, ROWS, HD), BF16),
            vmem((2, SEQ, HD), BF16),
            vmem((SEQ, QCOLS), BF16),
            vmem((256, SEQ), BF16),
            vmem((CHUNKS, SEQ, CW), BF16),
            vmem((CHUNKS, 256, CW), BF16),
            vmem((CHUNKS, ROWS, CW), BF16),
            vmem((CHUNKS, ROWS, CW), BF16),
            vmem((CHUNKS, ROWS, CW), BF16),
            vmem((NY, CHUNKS, CW), F32),
            vmem((NZ, CHUNKS, CW), F32),
            vmem((8, CHUNKS, CW), F32),
            dma((10,)), dma((32,)), dma((2,)), dma((8,)), dma((2,)), dma((CHUNKS,)), dma((CHUNKS + 1,)),
            dma((4,)), dma, dma((4,)), dma((CHUNKS,)), dma((CHUNKS,)), dma((CHUNKS,)),
            dma((3,)), dma((12,)), pltpu.SemaphoreType.REGULAR((6,)),
        ],
        compiler_params=pltpu.CompilerParams(
            collective_id=0, has_side_effects=True, vmem_limit_bytes=56 * 1024 * 1024
        ),
        name="sublayer",
    )(tokens[0], gain, bq, bkv, wq, wkv.T, wo, check_weights, cosine, sine)
    attended, total = pl.pallas_call(
        store_results,
        out_shape=(jax.ShapeDtypeStruct((ROWS, D), BF16), jax.ShapeDtypeStruct((1, D), F32)),
        in_specs=[inside, inside],
        out_specs=(anywhere, anywhere),
        scratch_shapes=[dma((2,))],
        name="store_results",
    )(
        pltpu.with_memory_space_constraint(attended, pltpu.VMEM),
        pltpu.with_memory_space_constraint(total, pltpu.VMEM),
    )
    return attended[None], total.reshape(D)


def solution(mesh):
    torus = Mesh(
        mesh.devices.reshape(8, 2, 4, 2, 2), ("dp_0", "dp_1", "tensor_0", "tensor_1", "tensor_2")
    )
    return jax.shard_map(
        local,
        mesh=torus,
        in_specs=(
            P(DP, TENSOR, None),
            P(),
            P(None, TENSOR),
            P(TENSOR),
            P(None, TENSOR),
            P(TENSOR),
            P(TENSOR, None),
            P(DP, None),
        ),
        out_specs=(P(DP, TENSOR, None), P()),
        check_vma=False,
    )
```

```python
import jax
import jax.numpy as jnp
import numpy as np
from jax import lax
from jax.experimental import pallas as pl
from jax.experimental.pallas import tpu as pltpu
from jax.sharding import Mesh
from jax.sharding import PartitionSpec as P

HD = 128
EPS = 1e-06
THETA = 1000000.0
TENSOR = ("tensor_0", "tensor_1", "tensor_2")
DP = ("dp_0", "dp_1")
MESH = pl.DeviceIdType.MESH
F32 = jnp.float32
BF16 = jnp.bfloat16

NY = 4
NZ = 8
D = 4096
ROWS = 64
QUARTER = 16
QCOLS = 256
SEQ = 1024
CHUNKS = 8
CW = D // CHUNKS
LATE = 4
NEAR_CHUNK = 7
(
    GATHER, SIBLING, SIBLING_WK, SIBLING_BIAS, WO, WO_SIBLING, MADE, MADE_HERE, MADE_SIBLING, CONTEXT, SUM, CHECK,
) = range(12)


def mult(value, by):
    return pl.multiple_of(value, by)


def split3(value):
    hi = value.astype(BF16).astype(F32)
    rest = value - hi
    mid = rest.astype(BF16).astype(F32)
    low = (rest - mid).astype(BF16).astype(F32)
    row = lax.broadcasted_iota(jnp.int32, (16, value.shape[1]), 0)
    rows = jnp.where(row == 0, hi, jnp.where(row == 1, mid, jnp.where(row == 2, low, 0.0)))
    return rows.astype(BF16)


def kernel(
    tokens, gain_in, bq_in, bkv_in, wq, wkv, wo, weights, cos, sin,
    out, check,
    tok, gain_v, bq_v, bkv_v, weights_v, xg, wqv, wkfull, wkt, bmine, bpair, cosv, sinv, qb, kvs, kv,
    ctx, ctx4, wo4, pbuf, ra, rfb, rfa, cy, cz, cc,
    ld, agr, agd, wkr, wor, wod, kvr, kvd, cxr, rar, rbr, cdr, sent, chain,
):
    z = lax.axis_index("dp_0")
    xh = lax.axis_index("dp_1")
    y = lax.axis_index("tensor_0")
    x = lax.axis_index("tensor_1")
    c = lax.axis_index("tensor_2")
    slot = x * 2 + c
    other_x = (x + 1) % 2
    other_c = (c + 1) % 2

    def at(dy=0, dx=0, dc=0):
        return {"tensor_0": (y + dy) % NY, "tensor_1": (x + dx) % 2, "tensor_2": (c + dc) % 2}

    def unit(dy, dx):
        return ((y + dy) % NY) * 2 + (x + dx) % 2

    up, down, pair, sibling = at(dy=1), at(dy=3), at(dx=1), at(dc=1)
    far = {"dp_1": (xh + 1) % 2, "tensor_1": other_x}

    contract_last = (((1,), (1,)), ((), ()))
    loads = {}

    def load(name, src, dst, sem):
        loads[name] = pltpu.make_async_copy(src, dst, sem)
        loads[name].start()

    load("tok", tokens, tok, ld.at[0])
    load("gain", gain_in, gain_v, ld.at[1])

    barrier = pltpu.get_barrier_semaphore()
    peers = (up, down, pair, sibling, far)

    def greet(sem_up, sem_down, distance):
        @pl.when(z + distance < NZ)
        def _():
            pl.semaphore_signal(sem_up, inc=1, device_id={"dp_0": (z + distance) % NZ}, device_id_type=MESH)

        @pl.when(z >= distance)
        def _():
            pl.semaphore_signal(sem_down, inc=1, device_id={"dp_0": (z + NZ - distance) % NZ}, device_id_type=MESH)

    def greet_round(r):
        greet(chain.at[2 * r], chain.at[2 * r + 1], 2 ** r)

    def greeted_round(r):
        distance = 2 ** r

        @pl.when(z >= distance)
        def _():
            pl.semaphore_wait(chain.at[2 * r], 1)

        @pl.when(z + distance < NZ)
        def _():
            pl.semaphore_wait(chain.at[2 * r + 1], 1)

    for peer in peers:
        pl.semaphore_signal(barrier, inc=1, device_id=peer, device_id_type=MESH)
    greet(barrier, barrier, 1)

    my_wk = wkfull.at[pl.ds(mult(c * 64, 64), 64), :]
    for k, (name, src, dst) in enumerate((
        ("bkv", bkv_in, bkv_v), ("wk", wkv, my_wk),
        ("bq", bq_in, bq_v), ("weights", weights, weights_v), ("wq", wq, wqv), ("cos", cos, cosv), ("sin", sin, sinv),
    )):
        load(name, src, dst, ld.at[2 + k])
    my_wo = pl.ds(mult(slot * QCOLS, QCOLS), QCOLS)
    for j in range(CHUNKS):
        pltpu.make_async_copy(wo.at[:, pl.ds(j * CW, CW)], wo4.at[j, my_wo, :], ld.at[9]).start()

    def send(src, dst, group, rsem, device):
        copy = pltpu.make_async_remote_copy(
            src_ref=src, dst_ref=dst, send_sem=sent.at[group], recv_sem=rsem,
            device_id=device, device_id_type=MESH,
        )
        copy.start()

    def all_sent(group, size):
        pltpu.make_async_remote_copy(
            src_ref=size, dst_ref=size, send_sem=sent.at[group], recv_sem=agr.at[0],
            device_id=sibling, device_id_type=MESH,
        ).wait_send()

    def arrived(dst, rsem):
        pltpu.make_async_remote_copy(
            src_ref=dst, dst_ref=dst, send_sem=sent.at[0], recv_sem=rsem,
            device_id=sibling, device_id_type=MESH,
        ).wait_recv()

    base = (y * 4 + slot) * ROWS
    loads["tok"].wait()
    loads["gain"].wait()
    gain = gain_v[...].astype(F32).reshape(1, D)

    def normalise(*quarters):
        for q in quarters:
            part = tok[q * QUARTER:(q + 1) * QUARTER, :].astype(F32)
            mean = jnp.mean(part * part, axis=-1, keepdims=True)
            xg[pl.ds(mult(base + q * QUARTER, QUARTER), QUARTER), :] = (
                part * lax.rsqrt(mean + EPS) * gain
            ).astype(BF16)

    normalise(0, 2)
    pl.semaphore_wait(barrier, len(peers) + (z + NZ - 1) // NZ + (2 * NZ - 2 - z) // NZ)
    greet_round(0)

    def piece(u, q):
        return xg.at[pl.ds(mult(u * 128 + c * ROWS + q * QUARTER, QUARTER), QUARTER), :]

    def sibling_piece(u, q):
        return xg.at[pl.ds(mult(u * 128 + other_c * ROWS + q * QUARTER, QUARTER), QUARTER), :]

    def relay(u, q, device):
        send(piece(u, q), piece(u, q), GATHER, agr.at[u * 4 + q], device)

    def relay_sibling(u, q):
        send(piece(u, q), piece(u, q), SIBLING, agd.at[u], sibling)

    def wait_piece(u, q):
        arrived(piece(u, q), agr.at[u * 4 + q])

    def part_piece(u, q, side):
        rows = pl.ds(mult(u * 128 + c * ROWS + q * QUARTER, QUARTER), QUARTER)
        return xg.at[rows, (D // 4 if side else 0):(D if side else D // 4)]

    def relay_part(u, q, side, device):
        send(part_piece(u, q, side), part_piece(u, q, side), GATHER, agr.at[u * 4 + q], device)

    def wait_sibling(u):
        arrived(xg.at[plane_rows(u, other_c), :], agd.at[u])

    def plane_rows(u, plane):
        return pl.ds(mult(u * 128 + plane * ROWS, ROWS), ROWS)

    own = unit(0, 0)
    for s in range(4):
        if s == 1:
            normalise(1, 3)
        if s < 3:
            relay(own, s, up)
            relay(own, (s + 2) % 4, down)
        relay(own, s, pair)
    for q in range(4):
        relay_sibling(own, q)

    loads["wk"].wait()
    send(my_wk, my_wk, SIBLING_WK, wkr.at[0], sibling)
    loads["bkv"].wait()
    bias_mine = bkv_v[...].astype(F32).reshape(1, 64)
    bias_mine = jnp.concatenate([bias_mine, bias_mine], axis=1)
    bmine[...] = jnp.broadcast_to(bias_mine, (8, 128))
    send(bmine, bpair, SIBLING_BIAS, wkr.at[1], sibling)

    def wo_piece(j, owner):
        return wo4.at[j, pl.ds(mult(owner * QCOLS, QCOLS), QCOLS), :]

    pltpu.make_async_copy(wo4.at[:, my_wo, :], wo4.at[:, my_wo, :], ld.at[9]).wait()
    for j in range(CHUNKS):
        if j != NEAR_CHUNK:
            send(wo_piece(j, slot), wo_piece(j, slot), WO, wor.at[j], far)
        send(wo_piece(j, slot), wo_piece(j, slot), WO_SIBLING, wod.at[CHUNKS], sibling)

    def send_near_chunk(first, rows):
        part = wo4.at[NEAR_CHUNK, pl.ds(mult(slot * QCOLS + first, ROWS), rows), :]
        send(part, part, WO, wor.at[NEAR_CHUNK], pair)

    far_slot = other_x * 2 + c
    sibling_slot = x * 2 + other_c
    far_sibling_slot = other_x * 2 + other_c

    def forward_wo(j):
        arrived(wo_piece(j, far_slot), wor.at[j])
        send(wo_piece(j, far_slot), wo_piece(j, far_slot), WO_SIBLING, wod.at[j], sibling)

    arrived(wkfull.at[pl.ds(mult(other_c * 64, 64), 64), :], wkr.at[0])
    arrived(bpair, wkr.at[1])
    for i in range(8):
        cols = slice(i * 512, (i + 1) * 512)
        wkt[cols, :] = wkfull[:, cols].T
    first = c == 0
    lane = lax.broadcasted_iota(jnp.int32, (1, 128), 1)
    bias_theirs = bpair[0:1, :]
    low_half = lane < 64
    kv_bias = jnp.where(
        first,
        jnp.where(low_half, bias_mine, bias_theirs),
        jnp.where(low_half, bias_theirs, bias_mine),
    )
    loads["bq"].wait()
    q_bias = bq_v[...].astype(F32).reshape(1, QCOLS)
    loads["wq"].wait()
    loads["cos"].wait()
    loads["sin"].wait()

    chip = y * 2 + x
    is_value = y // 2
    turned = (1 - is_value).astype(F32)
    straight = is_value.astype(F32)
    group = chip % NY
    local_user = group == y

    def rope(value, cosine, sine):
        return value * cosine + pltpu.roll(value, 64, 1) * sine

    def push(step, rows_kv, group, sem, device):
        return pltpu.make_async_remote_copy(
            src_ref=kvs.at[step], dst_ref=kv.at[is_value, rows_kv, :],
            send_sem=sent.at[group], recv_sem=sem, device_id=device, device_id_type=MESH,
        )

    def make_pairs(steps, units):
        lhs = [xg[plane_rows(u, c), :] for u in units]
        lhs = lhs[0] if len(lhs) == 1 else jnp.concatenate(lhs, axis=0)
        made_rows = jnp.dot(lhs, wkt[...], preferred_element_type=F32) + kv_bias
        made_rows = made_rows.astype(BF16).astype(F32)
        for i, (step, u) in enumerate(zip(steps, units)):
            rows_kv = plane_rows(u, c)
            cosine = cosv[rows_kv, :] * turned + straight
            sine = sinv[rows_kv, :] * turned
            result = rope(made_rows[i * ROWS:(i + 1) * ROWS, :], cosine, sine).astype(BF16)
            kvs[step] = result
            late = step >= LATE
            sem = kvr.at[is_value + (2 if late else 0)]

            @pl.when(local_user)
            def _():
                kv[is_value, rows_kv, :] = result

            @pl.when(jnp.logical_not(local_user))
            def _():
                push(step, rows_kv, MADE_HERE, sem, {"tensor_0": group}).start()

            push(step, rows_kv, MADE, sem, {"tensor_0": group, "tensor_1": other_x}).start()
            if late:
                for px in (other_x, x):
                    push(
                        step, rows_kv, MADE, kvd, {"tensor_0": group, "tensor_1": px, "tensor_2": other_c}
                    ).start()

    def make_query(units):
        lhs = [xg[pl.ds(mult(u * 128, 128), 128), :] for u in units]
        lhs = lhs[0] if len(lhs) == 1 else jnp.concatenate(lhs, axis=0)
        query = jnp.dot(lhs, wqv[...], preferred_element_type=F32) + q_bias
        for i, u in enumerate(units):
            rows = pl.ds(mult(u * 128, 128), 128)
            for h in range(2):
                cols = slice(h * HD, (h + 1) * HD)
                part = query[i * 128:(i + 1) * 128, cols]
                qb[rows, cols] = rope(part, cosv[rows, :], sinv[rows, :]).astype(BF16)

    def project(step, u):
        wait_sibling(u)
        make_pairs([step], [u])
        make_query([u])

    below, above, beside, across = unit(3, 0), unit(1, 0), unit(0, 1), unit(2, 0)
    x_across, x_below, x_above = unit(2, 1), unit(3, 1), unit(1, 1)

    greeted_round(0)
    greet_round(1)
    def relay_across(*quarters):
        for q in quarters:
            wait_piece(across, q)
            relay(across, q, pair)
            relay_sibling(across, q)

    def relay_beside(q):
        for device, halved in ((up, 0), (down, 2)):
            if q == halved:
                relay_part(beside, q, 0, device)
            else:
                relay(beside, q, device)

    for s in range(4):
        if s == 3:
            relay_across(0, 2)
        r = (s + 2) % 4
        wait_piece(below, s)
        wait_piece(above, r)
        if s < 2:
            relay(below, s, up)
            relay(above, r, down)
        if s == 0:
            relay(own, 3, up)
            relay(own, 1, down)
            relay_part(below, s, 1, pair)
            relay_part(above, r, 1, pair)
        wait_piece(beside, s)
        for q in ((), (0, 1), (2,), (3,))[s]:
            relay_beside(q)
        relay_sibling(below, s)
        relay_sibling(above, r)
        relay_sibling(beside, s)
    greeted_round(1)
    greet_round(2)

    def wait_x_neighbours(q):
        for u in (x_below, x_above):
            wait_piece(u, q)
            relay_sibling(u, q)

    def wait_x_across(*quarters):
        for q in quarters:
            wait_piece(x_across, q)
            relay_sibling(x_across, q)

    relay_across(1, 3)
    project(0, own)
    project(1, below)
    project(2, above)
    forward_wo(0)
    project(3, beside)
    wait_x_neighbours(0)
    forward_wo(1)
    wait_x_across(0, 2)
    wait_x_neighbours(1)
    greeted_round(2)
    project(4, across)
    forward_wo(2)
    wait_x_neighbours(2)
    wait_x_across(1, 3)
    make_pairs([5], [x_across])
    wait_x_neighbours(3)
    make_pairs([6, 7], [x_below, x_above])
    send_near_chunk(0, 192)

    made_here = [
        jnp.logical_and(y == 0, x == 0),
        jnp.logical_and(y == 3, x == 1),
    ]
    order = ((0, 0), (3, 0), (1, 0), (0, 1), (2, 0), (2, 1), (3, 1), (1, 1))

    def source_unit(kind, step):
        dy, dx = order[step]
        return ((kind * 2 + y // 2 + dy) % NY) * 2 + (y % 2 + dx) % 2

    def wait_made(kind, steps, late):
        @pl.when(jnp.logical_not(made_here[kind]))
        def _():
            arrived(kv.at[kind, 0:steps * ROWS, :], kvr.at[kind + 2 * late])

    def forward_made(kind):
        wait_made(kind, LATE, 0)
        for step in range(LATE):
            part = kv.at[kind, plane_rows(source_unit(kind, step), c), :]
            send(part, part, MADE_SIBLING, kvd, sibling)

    for kind in range(2):
        forward_made(kind)
    wait_sibling(x_across)
    make_query([x_across])
    forward_wo(3)
    wait_sibling(x_below)
    wait_sibling(x_above)
    make_query([x_below, x_above])
    for kind in range(2):
        wait_made(kind, 8 - LATE, 1)
    arrived(kv.at[0], kvd)

    scale = HD ** (-0.5)
    my_cols = pl.ds(mult(slot * QCOLS, QCOLS), QCOLS)
    beyond = ((1, 0), (1, 1), (0, 1))

    def theirs(dx, dc):
        return ((x + dx) % 2) * 2 + (c + dc) % 2

    def head_attention(v, h):
        block, before = slice(v * 256, (v + 1) * 256), slice(0, v * 256)
        row = lax.broadcasted_iota(jnp.int32, (256, 256), 0)
        col = lax.broadcasted_iota(jnp.int32, (256, 256), 1)
        cols = slice(h * HD, (h + 1) * HD)
        query = qb[block, cols]
        diagonal = lax.dot_general(query, kv[0, block, :], contract_last, preferred_element_type=F32)
        diagonal = jnp.where(row >= col, diagonal, -1e30)
        top = jnp.max(diagonal, axis=-1, keepdims=True)
        if v:
            earlier = lax.dot_general(query, kv[0, before, :], contract_last, preferred_element_type=F32)
            top = jnp.maximum(top, jnp.max(earlier, axis=-1, keepdims=True))
        weight = jnp.exp((diagonal - top) * scale)
        total = jnp.sum(weight, axis=-1, keepdims=True)
        mixed = jnp.dot(weight.astype(BF16), kv[1, block, :], preferred_element_type=F32)
        if v:
            weight = jnp.exp((earlier - top) * scale)
            total += jnp.sum(weight, axis=-1, keepdims=True)
            mixed += jnp.dot(weight.astype(BF16), kv[1, before, :], preferred_element_type=F32)
        ctx[block, cols] = (mixed / total).astype(BF16)

    def attend(k):
        b = (y + (2, 1, 3, 0)[k]) % NY
        target = pl.ds(k * ROWS, ROWS)
        for h in range(2):
            for v in range(NY):
                @pl.when(b == v)
                def _(v=v, h=h):
                    head_attention(v, h)

            cols = slice(h * HD, (h + 1) * HD)
            head = pl.ds(mult(slot * QCOLS + h * HD, HD), HD)
            for dx, dc in beyond:
                send(
                    ctx.at[pl.ds(mult(b * 256 + theirs(dx, dc) * ROWS, ROWS), ROWS), cols],
                    ctx4.at[target, head],
                    CONTEXT, cxr.at[k], at(dx=dx, dc=dc),
                )
        ctx4[target, my_cols] = ctx[pl.ds(mult(b * 256 + slot * ROWS, ROWS), ROWS), :]

    def gathered(k):
        arrived(ctx.at[0:3 * ROWS, :], cxr.at[k])

    def line(axis, index, size):
        return [{axis: (index + d) % size} for d in range(1, size)]

    cross = [
        {"dp_1": (xh + dh) % 2, "tensor_1": (x + dx) % 2, "tensor_2": (c + dc) % 2}
        for dh in range(2) for dx in range(2) for dc in range(2) if dh or dx or dc
    ]
    stages = [
        (line("tensor_0", y, NY), cy, y),
        (line("dp_0", z, NZ), cz, z),
        (cross, cc, xh * 4 + slot),
    ]

    def stage_start(i):
        devices, buf, index = stages[i]
        for device in devices:
            send(buf.at[index], buf.at[index], CHECK, cdr.at[i], device)

    def stage_end(i):
        devices, buf, _ = stages[i]
        arrived(buf.at[0:len(devices)], cdr.at[i])
        total = buf[0]
        for k in range(1, len(devices) + 1):
            total = total + buf[k]
        if i + 1 < len(stages):
            stages[i + 1][1][stages[i + 1][2]] = total
        else:
            total = total * (1.0 / 128.0)
            for j in range(CHUNKS):
                check[0:1, j * CW:(j + 1) * CW] = total[j:j + 1, :]

    attend(0)
    forward_wo(4)
    attend(1)
    send_near_chunk(192, 64)
    forward_wo(5)
    attend(2)
    attend(3)
    gathered(0)

    far_rows, up_rows, down_rows, own_rows = (slice(k * ROWS, (k + 1) * ROWS) for k in range(4))
    arrived(wo4.at[:, pl.ds(mult(sibling_slot * QCOLS, QCOLS), QCOLS), :], wod.at[CHUNKS])

    def far_target(j):
        arrived(wo_piece(j, far_sibling_slot), wod.at[j])
        product = jnp.dot(ctx4[far_rows, :], wo4[j], preferred_element_type=F32)
        pbuf[j, far_rows, :] = product.astype(BF16)
        send(pbuf.at[j, far_rows, :], ra.at[j], SUM, rar.at[j], down if j % 2 else up)

    def near_targets(j):
        product = jnp.dot(ctx4[ROWS:256, :], wo4[j], preferred_element_type=F32)
        pbuf[j, ROWS:256, :] = product.astype(BF16)
        if j % 2 == 0:
            send(pbuf.at[j, down_rows, :], rfa.at[j], SUM, rbr.at[j], down)
        else:
            send(pbuf.at[j, up_rows, :], rfb.at[j], SUM, rbr.at[j], up)

    def relay_sum(j):
        rows = up_rows if j % 2 == 0 else down_rows
        arrived(ra.at[j], rar.at[j])
        pbuf[j, rows, :] = (pbuf[j, rows, :].astype(F32) + ra[j].astype(F32)).astype(BF16)
        if j % 2 == 0:
            send(pbuf.at[j, rows, :], rfb.at[j], SUM, rbr.at[j], up)
        else:
            send(pbuf.at[j, rows, :], rfa.at[j], SUM, rbr.at[j], down)

    for j in range(2):
        far_target(j)
    loads["weights"].wait()
    summary = jnp.dot(split3(weights_v[...]), ctx[...], preferred_element_type=F32)
    summary = split3(jnp.sum(summary, axis=0, keepdims=True))
    for j in range(CHUNKS):
        term = jnp.dot(summary, wo4[j, my_cols, :], preferred_element_type=F32)
        cy[y, j:j + 1, :] = jnp.sum(term, axis=0, keepdims=True)
    stage_start(0)
    for j in range(2, 6):
        far_target(j)
    forward_wo(7)
    forward_wo(6)
    far_target(7)
    far_target(6)
    stage_end(0)
    stage_start(1)
    for k in range(1, 4):
        gathered(k)
    for j in range(CHUNKS):
        near_targets(j)
    for j in range(CHUNKS):
        relay_sum(j)
    stage_end(1)
    stage_start(2)
    for j in range(CHUNKS):
        arrived(pbuf.at[j, 0:2 * ROWS, :], rbr.at[j])
        total = pbuf[j, own_rows, :].astype(F32) + rfb[j].astype(F32) + rfa[j].astype(F32)
        cols = slice(j * CW, (j + 1) * CW)
        out[:, cols] = total.astype(BF16)

    stage_end(2)

    all_sent(GATHER, xg.at[0:28 * QUARTER, :])
    all_sent(SIBLING, xg.at[0:32 * QUARTER, :])
    all_sent(SIBLING_WK, my_wk)
    all_sent(SIBLING_BIAS, bmine)
    all_sent(WO, wo4.at[:, 0:QCOLS, :])
    all_sent(WO_SIBLING, wo4.at[:, 0:2 * QCOLS, :])
    all_sent(MADE, kv.at[0, 0:(24 - 2 * LATE) * ROWS, :])
    all_sent(MADE_SIBLING, kv.at[:, 0:LATE * ROWS, :])
    all_sent(CONTEXT, ctx.at[0:12 * ROWS, :])
    all_sent(SUM, xg.at[0:192, :])
    all_sent(CHECK, wo4.at[0, 0:17 * 16, :])

    @pl.when(jnp.logical_not(local_user))
    def _():
        all_sent(MADE_HERE, kv.at[0, 0:8 * ROWS, :])


def store_results(attended, total, out, check, sem):
    copies = (pltpu.make_async_copy(total, check, sem.at[1]), pltpu.make_async_copy(attended, out, sem.at[0]))
    for copy in copies:
        copy.start()
    for copy in copies:
        copy.wait()


def tables():
    half = HD // 2
    inverse = THETA ** (-(np.arange(half, dtype=np.float64) * 2.0 / HD))
    angles = np.arange(SEQ, dtype=np.float64)[:, None] * inverse[None, :]
    cosine, sine = np.cos(angles), np.sin(angles)
    return (
        np.concatenate([cosine, cosine], axis=1).astype(np.float32),
        np.concatenate([-sine, sine], axis=1).astype(np.float32),
    )


def local(tokens, gain, wq, bq, wkv, bkv, wo, check_weights):
    cosine, sine = tables()
    dma = pltpu.SemaphoreType.DMA
    vmem = pltpu.VMEM
    anywhere = pl.BlockSpec(memory_space=pl.ANY)
    inside = pl.BlockSpec(memory_space=pltpu.VMEM)
    attended, total = pl.pallas_call(
        kernel,
        out_shape=(
            pltpu.VMEM((ROWS, D), BF16),
            pltpu.VMEM((1, D), F32),
        ),
        in_specs=[anywhere] * 10,
        out_specs=(inside, inside),
        scratch_shapes=[
            vmem((ROWS, D), BF16),
            vmem((D,), BF16),
            vmem((QCOLS,), BF16),
            vmem((64,), BF16),
            vmem((1, SEQ), F32),
            vmem((SEQ, D), BF16),
            vmem((D, QCOLS), BF16),
            vmem((128, D), BF16),
            vmem((D, 128), BF16),
            vmem((8, 128), F32),
            vmem((8, 128), F32),
            vmem((SEQ, HD), F32),
            vmem((SEQ, HD), F32),
            vmem((SEQ, QCOLS), BF16),
            vmem((8, ROWS, HD), BF16),
            vmem((2, SEQ, HD), BF16),
            vmem((SEQ, QCOLS), BF16),
            vmem((256, SEQ), BF16),
            vmem((CHUNKS, SEQ, CW), BF16),
            vmem((CHUNKS, 256, CW), BF16),
            vmem((CHUNKS, ROWS, CW), BF16),
            vmem((CHUNKS, ROWS, CW), BF16),
            vmem((CHUNKS, ROWS, CW), BF16),
            vmem((NY, CHUNKS, CW), F32),
            vmem((NZ, CHUNKS, CW), F32),
            vmem((8, CHUNKS, CW), F32),
            dma((10,)), dma((32,)), dma((8,)), dma((2,)), dma((CHUNKS,)), dma((CHUNKS + 1,)),
            dma((4,)), dma, dma((4,)), dma((CHUNKS,)), dma((CHUNKS,)),
            dma((3,)), dma((12,)), pltpu.SemaphoreType.REGULAR((6,)),
        ],
        compiler_params=pltpu.CompilerParams(
            collective_id=0, has_side_effects=True, vmem_limit_bytes=56 * 1024 * 1024
        ),
        name="sublayer",
    )(tokens[0], gain, bq, bkv, wq, wkv.T, wo, check_weights, cosine, sine)
    attended, total = pl.pallas_call(
        store_results,
        out_shape=(jax.ShapeDtypeStruct((ROWS, D), BF16), jax.ShapeDtypeStruct((1, D), F32)),
        in_specs=[inside, inside],
        out_specs=(anywhere, anywhere),
        scratch_shapes=[dma((2,))],
        name="store_results",
    )(
        pltpu.with_memory_space_constraint(attended, pltpu.VMEM),
        pltpu.with_memory_space_constraint(total, pltpu.VMEM),
    )
    return attended[None], total.reshape(D)


def solution(mesh):
    torus = Mesh(
        mesh.devices.reshape(8, 2, 4, 2, 2), ("dp_0", "dp_1", "tensor_0", "tensor_1", "tensor_2")
    )
    return jax.shard_map(
        local,
        mesh=torus,
        in_specs=(
            P(DP, TENSOR, None),
            P(),
            P(None, TENSOR),
            P(TENSOR),
            P(None, TENSOR),
            P(TENSOR),
            P(TENSOR, None),
            P(DP, None),
        ),
        out_specs=(P(DP, TENSOR, None), P()),
        check_vma=False,
    )
```

```python
import jax
import jax.numpy as jnp
import numpy as np
from jax import lax
from jax.experimental import pallas as pl
from jax.experimental.pallas import tpu as pltpu
from jax.sharding import Mesh
from jax.sharding import PartitionSpec as P

HD = 128
EPS = 1e-06
THETA = 1000000.0
TENSOR = ("tensor_0", "tensor_1", "tensor_2")
DP = ("dp_0", "dp_1")
MESH = pl.DeviceIdType.MESH
F32 = jnp.float32
BF16 = jnp.bfloat16

NY = 4
NZ = 8
D = 4096
ROWS = 64
QUARTER = 16
QCOLS = 256
SEQ = 1024
CHUNKS = 8
CW = D // CHUNKS
LATE = 4
NEAR_CHUNK = 7
(
    GATHER, SIBLING, SIBLING_WK, SIBLING_BIAS, WO, WO_SIBLING, MADE, MADE_HERE, MADE_SIBLING, CONTEXT, SUM, CHECK,
) = range(12)


def mult(value, by):
    return pl.multiple_of(value, by)


def split3(value):
    hi = value.astype(BF16).astype(F32)
    rest = value - hi
    mid = rest.astype(BF16).astype(F32)
    low = (rest - mid).astype(BF16).astype(F32)
    row = lax.broadcasted_iota(jnp.int32, (16, value.shape[1]), 0)
    rows = jnp.where(row == 0, hi, jnp.where(row == 1, mid, jnp.where(row == 2, low, 0.0)))
    return rows.astype(BF16)


def kernel(
    tokens, gain_in, bq_in, bkv_in, wq, wkv, wo, weights, cos, sin,
    out, check,
    tok, gain_v, bq_v, bkv_v, weights_v, xg, wqv, wkfull, wkt, bmine, bpair, cosv, sinv, qb, kvs, kv,
    ctx, ctx4, wo4, pbuf, ra, rfb, rfa, cy, cz, cc,
    ld, agr, agd, wkr, wor, wod, kvr, kvd, cxr, rar, rbr, cdr, sent, chain,
):
    z = lax.axis_index("dp_0")
    xh = lax.axis_index("dp_1")
    y = lax.axis_index("tensor_0")
    x = lax.axis_index("tensor_1")
    c = lax.axis_index("tensor_2")
    slot = x * 2 + c
    other_x = (x + 1) % 2
    other_c = (c + 1) % 2

    def at(dy=0, dx=0, dc=0):
        return {"tensor_0": (y + dy) % NY, "tensor_1": (x + dx) % 2, "tensor_2": (c + dc) % 2}

    def unit(dy, dx):
        return ((y + dy) % NY) * 2 + (x + dx) % 2

    up, down, pair, sibling = at(dy=1), at(dy=3), at(dx=1), at(dc=1)
    far = {"dp_1": (xh + 1) % 2, "tensor_1": other_x}

    contract_last = (((1,), (1,)), ((), ()))
    loads = {}

    def load(name, src, dst, sem):
        loads[name] = pltpu.make_async_copy(src, dst, sem)
        loads[name].start()

    load("tok", tokens, tok, ld.at[0])
    load("gain", gain_in, gain_v, ld.at[1])

    barrier = pltpu.get_barrier_semaphore()
    peers = (up, down, pair, sibling, far)

    def greet(sem_up, sem_down, distance):
        @pl.when(z + distance < NZ)
        def _():
            pl.semaphore_signal(sem_up, inc=1, device_id={"dp_0": (z + distance) % NZ}, device_id_type=MESH)

        @pl.when(z >= distance)
        def _():
            pl.semaphore_signal(sem_down, inc=1, device_id={"dp_0": (z + NZ - distance) % NZ}, device_id_type=MESH)

    def greet_round(r):
        greet(chain.at[2 * r], chain.at[2 * r + 1], 2 ** r)

    def greeted_round(r):
        distance = 2 ** r

        @pl.when(z >= distance)
        def _():
            pl.semaphore_wait(chain.at[2 * r], 1)

        @pl.when(z + distance < NZ)
        def _():
            pl.semaphore_wait(chain.at[2 * r + 1], 1)

    for peer in peers:
        pl.semaphore_signal(barrier, inc=1, device_id=peer, device_id_type=MESH)
    greet(barrier, barrier, 1)

    my_wk = wkfull.at[pl.ds(mult(c * 64, 64), 64), :]
    for k, (name, src, dst) in enumerate((
        ("bkv", bkv_in, bkv_v), ("wk", wkv, my_wk),
        ("bq", bq_in, bq_v), ("weights", weights, weights_v), ("wq", wq, wqv), ("cos", cos, cosv), ("sin", sin, sinv),
    )):
        load(name, src, dst, ld.at[2 + k])
    my_wo = pl.ds(mult(slot * QCOLS, QCOLS), QCOLS)
    for j in range(CHUNKS):
        pltpu.make_async_copy(wo.at[:, pl.ds(j * CW, CW)], wo4.at[j, my_wo, :], ld.at[9]).start()

    def send(src, dst, group, rsem, device):
        copy = pltpu.make_async_remote_copy(
            src_ref=src, dst_ref=dst, send_sem=sent.at[group], recv_sem=rsem,
            device_id=device, device_id_type=MESH,
        )
        copy.start()

    def all_sent(group, size):
        pltpu.make_async_remote_copy(
            src_ref=size, dst_ref=size, send_sem=sent.at[group], recv_sem=agr.at[0],
            device_id=sibling, device_id_type=MESH,
        ).wait_send()

    def arrived(dst, rsem):
        pltpu.make_async_remote_copy(
            src_ref=dst, dst_ref=dst, send_sem=sent.at[0], recv_sem=rsem,
            device_id=sibling, device_id_type=MESH,
        ).wait_recv()

    base = (y * 4 + slot) * ROWS
    loads["tok"].wait()
    loads["gain"].wait()
    gain = gain_v[...].astype(F32).reshape(1, D)

    def normalise(*quarters):
        for q in quarters:
            part = tok[q * QUARTER:(q + 1) * QUARTER, :].astype(F32)
            mean = jnp.mean(part * part, axis=-1, keepdims=True)
            xg[pl.ds(mult(base + q * QUARTER, QUARTER), QUARTER), :] = (
                part * lax.rsqrt(mean + EPS) * gain
            ).astype(BF16)

    normalise(0, 2)
    pl.semaphore_wait(barrier, len(peers) + (z + NZ - 1) // NZ + (2 * NZ - 2 - z) // NZ)
    greet_round(0)

    def piece(u, q):
        return xg.at[pl.ds(mult(u * 128 + c * ROWS + q * QUARTER, QUARTER), QUARTER), :]

    def sibling_piece(u, q):
        return xg.at[pl.ds(mult(u * 128 + other_c * ROWS + q * QUARTER, QUARTER), QUARTER), :]

    def relay(u, q, device):
        send(piece(u, q), piece(u, q), GATHER, agr.at[u * 4 + q], device)

    def relay_sibling(u, q):
        send(piece(u, q), piece(u, q), SIBLING, agd.at[u], sibling)

    def wait_piece(u, q):
        arrived(piece(u, q), agr.at[u * 4 + q])

    def part_piece(u, q, side):
        rows = pl.ds(mult(u * 128 + c * ROWS + q * QUARTER, QUARTER), QUARTER)
        return xg.at[rows, (D // 4 if side else 0):(D if side else D // 4)]

    def relay_part(u, q, side, device):
        send(part_piece(u, q, side), part_piece(u, q, side), GATHER, agr.at[u * 4 + q], device)

    def wait_sibling(u):
        arrived(xg.at[plane_rows(u, other_c), :], agd.at[u])

    def plane_rows(u, plane):
        return pl.ds(mult(u * 128 + plane * ROWS, ROWS), ROWS)

    own = unit(0, 0)
    for s in range(4):
        if s == 1:
            normalise(1, 3)
        if s < 3:
            relay(own, s, up)
            relay(own, (s + 2) % 4, down)
        relay(own, s, pair)
    for q in range(4):
        relay_sibling(own, q)

    loads["wk"].wait()
    send(my_wk, my_wk, SIBLING_WK, wkr.at[0], sibling)
    loads["bkv"].wait()
    bias_mine = bkv_v[...].astype(F32).reshape(1, 64)
    bias_mine = jnp.concatenate([bias_mine, bias_mine], axis=1)
    bmine[...] = jnp.broadcast_to(bias_mine, (8, 128))
    send(bmine, bpair, SIBLING_BIAS, wkr.at[1], sibling)

    def wo_piece(j, owner):
        return wo4.at[j, pl.ds(mult(owner * QCOLS, QCOLS), QCOLS), :]

    pltpu.make_async_copy(wo4.at[:, my_wo, :], wo4.at[:, my_wo, :], ld.at[9]).wait()
    for j in range(CHUNKS):
        if j != NEAR_CHUNK:
            send(wo_piece(j, slot), wo_piece(j, slot), WO, wor.at[j], far)
        send(wo_piece(j, slot), wo_piece(j, slot), WO_SIBLING, wod.at[CHUNKS], sibling)

    def send_near_chunk(first, rows):
        part = wo4.at[NEAR_CHUNK, pl.ds(mult(slot * QCOLS + first, ROWS), rows), :]
        send(part, part, WO, wor.at[NEAR_CHUNK], pair)

    far_slot = other_x * 2 + c
    sibling_slot = x * 2 + other_c
    far_sibling_slot = other_x * 2 + other_c

    def forward_wo(j):
        arrived(wo_piece(j, far_slot), wor.at[j])
        send(wo_piece(j, far_slot), wo_piece(j, far_slot), WO_SIBLING, wod.at[j], sibling)

    arrived(wkfull.at[pl.ds(mult(other_c * 64, 64), 64), :], wkr.at[0])
    arrived(bpair, wkr.at[1])
    for i in range(8):
        cols = slice(i * 512, (i + 1) * 512)
        wkt[cols, :] = wkfull[:, cols].T
    first = c == 0
    lane = lax.broadcasted_iota(jnp.int32, (1, 128), 1)
    bias_theirs = bpair[0:1, :]
    low_half = lane < 64
    kv_bias = jnp.where(
        first,
        jnp.where(low_half, bias_mine, bias_theirs),
        jnp.where(low_half, bias_theirs, bias_mine),
    )
    loads["bq"].wait()
    q_bias = bq_v[...].astype(F32).reshape(1, QCOLS)
    loads["wq"].wait()
    loads["cos"].wait()
    loads["sin"].wait()

    chip = y * 2 + x
    is_value = y // 2
    turned = (1 - is_value).astype(F32)
    straight = is_value.astype(F32)
    group = chip % NY
    local_user = group == y

    def rope(value, cosine, sine):
        return value * cosine + pltpu.roll(value, 64, 1) * sine

    def push(step, rows_kv, group, sem, device):
        return pltpu.make_async_remote_copy(
            src_ref=kvs.at[step], dst_ref=kv.at[is_value, rows_kv, :],
            send_sem=sent.at[group], recv_sem=sem, device_id=device, device_id_type=MESH,
        )

    def make_pairs(steps, units):
        lhs = [xg[plane_rows(u, c), :] for u in units]
        lhs = lhs[0] if len(lhs) == 1 else jnp.concatenate(lhs, axis=0)
        made_rows = jnp.dot(lhs, wkt[...], preferred_element_type=F32) + kv_bias
        made_rows = made_rows.astype(BF16).astype(F32)
        for i, (step, u) in enumerate(zip(steps, units)):
            rows_kv = plane_rows(u, c)
            cosine = cosv[rows_kv, :] * turned + straight
            sine = sinv[rows_kv, :] * turned
            result = rope(made_rows[i * ROWS:(i + 1) * ROWS, :], cosine, sine).astype(BF16)
            kvs[step] = result
            late = step >= LATE
            sem = kvr.at[is_value + (2 if late else 0)]

            @pl.when(local_user)
            def _():
                kv[is_value, rows_kv, :] = result

            @pl.when(jnp.logical_not(local_user))
            def _():
                push(step, rows_kv, MADE_HERE, sem, {"tensor_0": group}).start()

            push(step, rows_kv, MADE, sem, {"tensor_0": group, "tensor_1": other_x}).start()
            if late:
                for px in (other_x, x):
                    push(
                        step, rows_kv, MADE, kvd, {"tensor_0": group, "tensor_1": px, "tensor_2": other_c}
                    ).start()

    def make_query(units):
        lhs = [xg[pl.ds(mult(u * 128, 128), 128), :] for u in units]
        lhs = lhs[0] if len(lhs) == 1 else jnp.concatenate(lhs, axis=0)
        query = jnp.dot(lhs, wqv[...], preferred_element_type=F32) + q_bias
        for i, u in enumerate(units):
            rows = pl.ds(mult(u * 128, 128), 128)
            for h in range(2):
                cols = slice(h * HD, (h + 1) * HD)
                part = query[i * 128:(i + 1) * 128, cols]
                qb[rows, cols] = rope(part, cosv[rows, :], sinv[rows, :]).astype(BF16)

    def project(step, u):
        wait_sibling(u)
        make_pairs([step], [u])
        make_query([u])

    below, above, beside, across = unit(3, 0), unit(1, 0), unit(0, 1), unit(2, 0)
    x_across, x_below, x_above = unit(2, 1), unit(3, 1), unit(1, 1)

    greeted_round(0)
    greet_round(1)
    def relay_across(*quarters):
        for q in quarters:
            wait_piece(across, q)
            relay(across, q, pair)
            relay_sibling(across, q)

    def relay_beside(q):
        for device, halved in ((up, 0), (down, 2)):
            if q == halved:
                relay_part(beside, q, 0, device)
            else:
                relay(beside, q, device)

    for s in range(4):
        if s == 3:
            relay_across(0, 2)
        r = (s + 2) % 4
        wait_piece(below, s)
        wait_piece(above, r)
        if s < 2:
            relay(below, s, up)
            relay(above, r, down)
        if s == 0:
            relay(own, 3, up)
            relay(own, 1, down)
            relay_part(below, s, 1, pair)
            relay_part(above, r, 1, pair)
        wait_piece(beside, s)
        for q in ((), (0, 1), (2,), (3,))[s]:
            relay_beside(q)
        relay_sibling(below, s)
        relay_sibling(above, r)
        relay_sibling(beside, s)
    greeted_round(1)
    greet_round(2)

    def wait_x_neighbours(q):
        for u in (x_below, x_above):
            wait_piece(u, q)
            relay_sibling(u, q)

    def wait_x_across(*quarters):
        for q in quarters:
            wait_piece(x_across, q)
            relay_sibling(x_across, q)

    relay_across(1, 3)
    project(0, own)
    project(1, below)
    project(2, above)
    forward_wo(0)
    project(3, beside)
    wait_x_neighbours(0)
    forward_wo(1)
    wait_x_across(0, 2)
    wait_x_neighbours(1)
    greeted_round(2)
    project(4, across)
    forward_wo(2)
    wait_x_neighbours(2)
    wait_x_across(1, 3)
    make_pairs([5], [x_across])
    wait_x_neighbours(3)
    make_pairs([6, 7], [x_below, x_above])
    send_near_chunk(0, 192)

    made_here = [
        jnp.logical_and(y == 0, x == 0),
        jnp.logical_and(y == 3, x == 1),
    ]
    order = ((0, 0), (3, 0), (1, 0), (0, 1), (2, 0), (2, 1), (3, 1), (1, 1))

    def source_unit(kind, step):
        dy, dx = order[step]
        return ((kind * 2 + y // 2 + dy) % NY) * 2 + (y % 2 + dx) % 2

    def wait_made(kind, steps, late):
        @pl.when(jnp.logical_not(made_here[kind]))
        def _():
            arrived(kv.at[kind, 0:steps * ROWS, :], kvr.at[kind + 2 * late])

    def forward_made(kind):
        wait_made(kind, LATE, 0)
        for step in range(LATE):
            part = kv.at[kind, plane_rows(source_unit(kind, step), c), :]
            send(part, part, MADE_SIBLING, kvd, sibling)

    for kind in range(2):
        forward_made(kind)
    wait_sibling(x_across)
    make_query([x_across])
    forward_wo(3)
    wait_sibling(x_below)
    wait_sibling(x_above)
    make_query([x_below, x_above])
    for kind in range(2):
        wait_made(kind, 8 - LATE, 1)
    arrived(kv.at[0], kvd)

    scale = HD ** (-0.5)
    my_cols = pl.ds(mult(slot * QCOLS, QCOLS), QCOLS)
    beyond = ((1, 0), (1, 1), (0, 1))

    def theirs(dx, dc):
        return ((x + dx) % 2) * 2 + (c + dc) % 2

    def attention(v, start, count):
        block, before = slice(v * 256, (v + 1) * 256), slice(0, v * 256)
        rows = pl.ds(mult(v * 256 + start, 128), count)
        row = lax.broadcasted_iota(jnp.int32, (count, 256), 0) + start
        col = lax.broadcasted_iota(jnp.int32, (count, 256), 1)
        for h in range(2):
            cols = slice(h * HD, (h + 1) * HD)
            query = qb[rows, cols]
            diagonal = lax.dot_general(query, kv[0, block, :], contract_last, preferred_element_type=F32)
            diagonal = jnp.where(row >= col, diagonal, -1e30)
            top = jnp.max(diagonal, axis=-1, keepdims=True)
            if v:
                earlier = lax.dot_general(query, kv[0, before, :], contract_last, preferred_element_type=F32)
                top = jnp.maximum(top, jnp.max(earlier, axis=-1, keepdims=True))
            weight = jnp.exp((diagonal - top) * scale)
            total = jnp.sum(weight, axis=-1, keepdims=True)
            mixed = jnp.dot(weight.astype(BF16), kv[1, block, :], preferred_element_type=F32)
            if v:
                weight = jnp.exp((earlier - top) * scale)
                total += jnp.sum(weight, axis=-1, keepdims=True)
                mixed += jnp.dot(weight.astype(BF16), kv[1, before, :], preferred_element_type=F32)
            ctx[rows, cols] = (mixed / total).astype(BF16)

    def attend(k):
        b = (y + (2, 1, 3, 0)[k]) % NY
        target = pl.ds(k * ROWS, ROWS)

        def part(start, count, users):
            for v in range(NY):
                @pl.when(b == v)
                def _(v=v):
                    attention(v, start, count)

            for dx, dc in users:
                send(
                    ctx.at[pl.ds(mult(b * 256 + theirs(dx, dc) * ROWS, ROWS), ROWS), :],
                    ctx4.at[target, my_cols],
                    CONTEXT, cxr.at[k], at(dx=dx, dc=dc),
                )

        if k == 0:
            part(other_x * 128, 128, beyond[:2])
            part(x * 128, 128, beyond[2:])
        else:
            part(0, 256, beyond)
        ctx4[target, my_cols] = ctx[pl.ds(mult(b * 256 + slot * ROWS, ROWS), ROWS), :]

    def gathered(k):
        arrived(ctx.at[0:3 * ROWS, :], cxr.at[k])

    def line(axis, index, size):
        return [{axis: (index + d) % size} for d in range(1, size)]

    cross = [
        {"dp_1": (xh + dh) % 2, "tensor_1": (x + dx) % 2, "tensor_2": (c + dc) % 2}
        for dh in range(2) for dx in range(2) for dc in range(2) if dh or dx or dc
    ]
    stages = [
        (line("tensor_0", y, NY), cy, y),
        (line("dp_0", z, NZ), cz, z),
        (cross, cc, xh * 4 + slot),
    ]

    def stage_start(i):
        devices, buf, index = stages[i]
        for device in devices:
            send(buf.at[index], buf.at[index], CHECK, cdr.at[i], device)

    def stage_end(i):
        devices, buf, _ = stages[i]
        arrived(buf.at[0:len(devices)], cdr.at[i])
        total = buf[0]
        for k in range(1, len(devices) + 1):
            total = total + buf[k]
        if i + 1 < len(stages):
            stages[i + 1][1][stages[i + 1][2]] = total
        else:
            total = total * (1.0 / 128.0)
            for j in range(CHUNKS):
                check[0:1, j * CW:(j + 1) * CW] = total[j:j + 1, :]

    attend(0)
    forward_wo(4)
    attend(1)
    send_near_chunk(192, 64)
    forward_wo(5)
    attend(2)
    attend(3)
    gathered(0)

    far_rows, up_rows, down_rows, own_rows = (slice(k * ROWS, (k + 1) * ROWS) for k in range(4))
    arrived(wo4.at[:, pl.ds(mult(sibling_slot * QCOLS, QCOLS), QCOLS), :], wod.at[CHUNKS])

    def far_target(j):
        arrived(wo_piece(j, far_sibling_slot), wod.at[j])
        product = jnp.dot(ctx4[far_rows, :], wo4[j], preferred_element_type=F32)
        pbuf[j, far_rows, :] = product.astype(BF16)
        send(pbuf.at[j, far_rows, :], ra.at[j], SUM, rar.at[j], down if j % 2 else up)

    def near_targets(j):
        product = jnp.dot(ctx4[ROWS:256, :], wo4[j], preferred_element_type=F32)
        pbuf[j, ROWS:256, :] = product.astype(BF16)
        if j % 2 == 0:
            send(pbuf.at[j, down_rows, :], rfa.at[j], SUM, rbr.at[j], down)
        else:
            send(pbuf.at[j, up_rows, :], rfb.at[j], SUM, rbr.at[j], up)

    def relay_sum(j):
        rows = up_rows if j % 2 == 0 else down_rows
        arrived(ra.at[j], rar.at[j])
        pbuf[j, rows, :] = (pbuf[j, rows, :].astype(F32) + ra[j].astype(F32)).astype(BF16)
        if j % 2 == 0:
            send(pbuf.at[j, rows, :], rfb.at[j], SUM, rbr.at[j], up)
        else:
            send(pbuf.at[j, rows, :], rfa.at[j], SUM, rbr.at[j], down)

    for j in range(2):
        far_target(j)
    loads["weights"].wait()
    summary = jnp.dot(split3(weights_v[...]), ctx[...], preferred_element_type=F32)
    summary = split3(jnp.sum(summary, axis=0, keepdims=True))
    for j in range(CHUNKS):
        term = jnp.dot(summary, wo4[j, my_cols, :], preferred_element_type=F32)
        cy[y, j:j + 1, :] = jnp.sum(term, axis=0, keepdims=True)
    stage_start(0)
    for j in range(2, 6):
        far_target(j)
    forward_wo(7)
    forward_wo(6)
    stage_end(0)
    stage_start(1)
    for k in range(1, 4):
        gathered(k)
    for j in range(4):
        near_targets(j)
    far_target(7)
    far_target(6)
    for j in range(4, CHUNKS):
        near_targets(j)
    for j in range(CHUNKS):
        relay_sum(j)
    stage_end(1)
    stage_start(2)
    for j in range(CHUNKS):
        arrived(pbuf.at[j, 0:2 * ROWS, :], rbr.at[j])
        total = pbuf[j, own_rows, :].astype(F32) + rfb[j].astype(F32) + rfa[j].astype(F32)
        cols = slice(j * CW, (j + 1) * CW)
        out[:, cols] = total.astype(BF16)

    stage_end(2)

    all_sent(GATHER, xg.at[0:28 * QUARTER, :])
    all_sent(SIBLING, xg.at[0:32 * QUARTER, :])
    all_sent(SIBLING_WK, my_wk)
    all_sent(SIBLING_BIAS, bmine)
    all_sent(WO, wo4.at[:, 0:QCOLS, :])
    all_sent(WO_SIBLING, wo4.at[:, 0:2 * QCOLS, :])
    all_sent(MADE, kv.at[0, 0:(24 - 2 * LATE) * ROWS, :])
    all_sent(MADE_SIBLING, kv.at[:, 0:LATE * ROWS, :])
    all_sent(CONTEXT, ctx.at[0:12 * ROWS, :])
    all_sent(SUM, xg.at[0:192, :])
    all_sent(CHECK, wo4.at[0, 0:17 * 16, :])

    @pl.when(jnp.logical_not(local_user))
    def _():
        all_sent(MADE_HERE, kv.at[0, 0:8 * ROWS, :])


def store_results(attended, total, out, check, sem):
    copies = (pltpu.make_async_copy(total, check, sem.at[1]), pltpu.make_async_copy(attended, out, sem.at[0]))
    for copy in copies:
        copy.start()
    for copy in copies:
        copy.wait()


def tables():
    half = HD // 2
    inverse = THETA ** (-(np.arange(half, dtype=np.float64) * 2.0 / HD))
    angles = np.arange(SEQ, dtype=np.float64)[:, None] * inverse[None, :]
    cosine, sine = np.cos(angles), np.sin(angles)
    return (
        np.concatenate([cosine, cosine], axis=1).astype(np.float32),
        np.concatenate([-sine, sine], axis=1).astype(np.float32),
    )


def local(tokens, gain, wq, bq, wkv, bkv, wo, check_weights):
    cosine, sine = tables()
    dma = pltpu.SemaphoreType.DMA
    vmem = pltpu.VMEM
    anywhere = pl.BlockSpec(memory_space=pl.ANY)
    inside = pl.BlockSpec(memory_space=pltpu.VMEM)
    attended, total = pl.pallas_call(
        kernel,
        out_shape=(
            pltpu.VMEM((ROWS, D), BF16),
            pltpu.VMEM((1, D), F32),
        ),
        in_specs=[anywhere] * 10,
        out_specs=(inside, inside),
        scratch_shapes=[
            vmem((ROWS, D), BF16),
            vmem((D,), BF16),
            vmem((QCOLS,), BF16),
            vmem((64,), BF16),
            vmem((1, SEQ), F32),
            vmem((SEQ, D), BF16),
            vmem((D, QCOLS), BF16),
            vmem((128, D), BF16),
            vmem((D, 128), BF16),
            vmem((8, 128), F32),
            vmem((8, 128), F32),
            vmem((SEQ, HD), F32),
            vmem((SEQ, HD), F32),
            vmem((SEQ, QCOLS), BF16),
            vmem((8, ROWS, HD), BF16),
            vmem((2, SEQ, HD), BF16),
            vmem((SEQ, QCOLS), BF16),
            vmem((256, SEQ), BF16),
            vmem((CHUNKS, SEQ, CW), BF16),
            vmem((CHUNKS, 256, CW), BF16),
            vmem((CHUNKS, ROWS, CW), BF16),
            vmem((CHUNKS, ROWS, CW), BF16),
            vmem((CHUNKS, ROWS, CW), BF16),
            vmem((NY, CHUNKS, CW), F32),
            vmem((NZ, CHUNKS, CW), F32),
            vmem((8, CHUNKS, CW), F32),
            dma((10,)), dma((32,)), dma((8,)), dma((2,)), dma((CHUNKS,)), dma((CHUNKS + 1,)),
            dma((4,)), dma, dma((4,)), dma((CHUNKS,)), dma((CHUNKS,)),
            dma((3,)), dma((12,)), pltpu.SemaphoreType.REGULAR((6,)),
        ],
        compiler_params=pltpu.CompilerParams(
            collective_id=0, has_side_effects=True, vmem_limit_bytes=56 * 1024 * 1024
        ),
        name="sublayer",
    )(tokens[0], gain, bq, bkv, wq, wkv.T, wo, check_weights, cosine, sine)
    attended, total = pl.pallas_call(
        store_results,
        out_shape=(jax.ShapeDtypeStruct((ROWS, D), BF16), jax.ShapeDtypeStruct((1, D), F32)),
        in_specs=[inside, inside],
        out_specs=(anywhere, anywhere),
        scratch_shapes=[dma((2,))],
        name="store_results",
    )(
        pltpu.with_memory_space_constraint(attended, pltpu.VMEM),
        pltpu.with_memory_space_constraint(total, pltpu.VMEM),
    )
    return attended[None], total.reshape(D)


def solution(mesh):
    torus = Mesh(
        mesh.devices.reshape(8, 2, 4, 2, 2), ("dp_0", "dp_1", "tensor_0", "tensor_1", "tensor_2")
    )
    return jax.shard_map(
        local,
        mesh=torus,
        in_specs=(
            P(DP, TENSOR, None),
            P(),
            P(None, TENSOR),
            P(TENSOR),
            P(None, TENSOR),
            P(TENSOR),
            P(TENSOR, None),
            P(DP, None),
        ),
        out_specs=(P(DP, TENSOR, None), P()),
        check_vma=False,
    )
```
